32 devices in a mesh: ka: 4 (over x, core), rows: 8 (over z, y).
Axes of the slice: x: 2, y: 2, z: 4, core: 2. Of those that a mesh axis runs over, the one named last changes fastest.
Arguments:
- hoppings: bfloat16 [8, 384, 128, 128], P('rows', 'ka'), may hold values from -0.09375 to 0.09375
- tile_rows: int32 [8, 384], P('rows', 'ka'), may hold values from 0 to 95, as said below
- tile_cols: int32 [8, 384], P('rows', 'ka'), may hold values from 0 to 95, as said below
- tile_lats: int32 [8, 384], P('rows', 'ka'), may hold values from 0 to 8
- tile_counts: int32 [8, 4], P('rows', 'ka'), may hold values from 48 to 96, as said below
- phase_angle: float32 [8, 9], P('ka'), may hold values from -3.140625 to 3.140625
- vectors: bfloat16 [8, 2, 12288, 256], P('ka', None, 'rows'), may hold values from -6 to 6
Outputs:
- bloch_product: float32 [8, 2, 12288, 256], P('ka', None, 'rows')
The draws below stay inside these ranges and needn't reach their ends.
Inputs may be any that keep to these rules, and one draw needn't show every extreme that they name: `tile_rows`: slots of row block r (first index) hold tile rows r * 12 to (r + 1) * 12 - 1; several slots may name the same block. `tile_cols`: the cyclic distance between a slot's tile column and its tile row is at most 16, and both distances 16 occur in every row block. `tile_counts`: the live slots of a device are the first ones of its part of the list; some device has all 96 live.
All inputs are finite; a program needn't handle non-finite values.
Results may differ from the reference program's by a relative error of at most 0.0029.
Values may be sent and summed in bfloat16 or wider, within the bound.
A program may use at most 320 MiB of HBM per device.

```python
import jax
import jax.numpy as jnp
from jax import lax

TS = 128
TORB = 96
NLAT = 9
BAND = 16
NVEC = 256
TILE_DEV = 96
TR = 12
LISTS = 384
ORB = 12288
KPTS = 8
N_KA = 4
N_ROWS = 8


def tile_coordinates(key):
    folded_rows = jax.random.fold_in(key, 17)
    first_key, second_key = jax.random.split(folded_rows)
    row_position = jax.random.randint(first_key, (N_ROWS, TILE_DEV * N_KA), 0, TR)
    row_position = row_position + (jnp.arange(N_ROWS, dtype=jnp.int32) * TR)[:, None]
    column_step = jax.random.randint(second_key, (N_ROWS, TILE_DEV * N_KA), -BAND, BAND + 1)
    column_step = column_step.at[:, 0].set(BAND).at[:, 1].set(-BAND)
    col_index = jnp.mod(row_position + column_step, TORB)
    return (row_position.astype(jnp.int32), col_index.astype(jnp.int32))


def draw_tile_rows(key, part):
    return tile_coordinates(key)[0]


def draw_tile_cols(key, part):
    return tile_coordinates(key)[1]


def draw_tile_counts(key, part):
    folded_rows = jax.random.fold_in(key, 29)
    first_key, second_key = jax.random.split(folded_rows)
    counts = jax.random.randint(first_key, (N_ROWS * N_KA,), (TILE_DEV + 1) // 2, TILE_DEV + 1)
    full_slot = jax.random.randint(second_key, (), 0, N_ROWS * N_KA)
    counts = counts.at[full_slot].set(TILE_DEV)
    return counts.reshape(N_ROWS, N_KA).astype(jnp.int32)


def plant(result, rng, low, largest):
    longest = result.shape.index(max(result.shape))
    spots = []
    for shift in (0, 1):
        where = [jax.random.randint(jax.random.fold_in(rng, axis), (), 0, length) for axis, length in enumerate(result.shape)]
        where[longest] = (where[longest] + shift) % result.shape[longest]
        spots.append(tuple(where))
    return result.at[spots[0]].set(low).at[spots[1]].set(largest)


def shard_levels(key, extent, cuts, least, high):
    def one(dim, parts):
        steps = jax.random.uniform(jax.random.fold_in(jax.random.fold_in(key, 6), dim), (parts,), jnp.float32, least / len(cuts), high / len(cuts))
        return jnp.repeat(jnp.exp(steps), extent[dim] // parts).reshape((-1,) + (1,) * (len(extent) - dim - 1))

    factor_of = one(*cuts[0])
    for cut in cuts[1:]:
        factor_of = factor_of * one(*cut)
    return factor_of


def centred(rng, dims, spread, most, cuts=(), held_as=jnp.bfloat16):
    result = jax.random.normal(rng, dims, jnp.float32) * spread
    if len(cuts) > 0:
        result = shard_levels(rng, dims, cuts, -0.22, 0.18) * result
    return jnp.clip(result, min=-most, max=most).astype(held_as)


def setup_inputs(seed: int = 0) -> dict:
    streams_of = jax.random.split(jax.random.key(seed), 8)
    return {
        "hoppings": centred(streams_of[0], (N_ROWS, LISTS, TS, TS), (TS * TILE_DEV * N_KA // TR) ** -0.5, 0.09375, ((0, 8), (1, 4))),
        "tile_rows": draw_tile_rows(jax.random.fold_in(streams_of[7], 71), 0),
        "tile_cols": draw_tile_cols(jax.random.fold_in(streams_of[7], 71), 0),
        "tile_lats": plant(jax.random.randint(streams_of[3], (N_ROWS, LISTS), 0, NLAT), jax.random.fold_in(streams_of[3], 1), 0, NLAT - 1).astype(jnp.int32),
        "tile_counts": draw_tile_counts(jax.random.fold_in(streams_of[7], 71), 0),
        "phase_angle": jnp.clip(jax.random.uniform(streams_of[5], (KPTS, NLAT), jnp.float32, -3.140625, 3.140625), -3.140625, 3.140625),
        "vectors": centred(streams_of[6], (KPTS, 2, ORB, NVEC), 1.0, 6.0, ((0, 4), (2, 8))),
    }


def reference(hoppings, tile_rows, tile_cols, tile_lats, tile_counts, phase_angle, vectors):
    list_count = hoppings.shape[1]
    slot_index = jnp.arange(list_count, dtype=jnp.int32)
    live_mask = (slot_index[None, :] % TILE_DEV) < tile_counts[:, slot_index // TILE_DEV]
    live_f32 = live_mask.astype(jnp.float32)
    block_ids = (tile_rows * TORB + tile_cols).astype(jnp.int32)

    def one_point(point_data):
        angles, point_vectors = point_data
        cos_weight = jnp.cos(angles)[tile_lats] * live_f32
        sin_weight = jnp.sin(angles)[tile_lats] * live_f32

        def add_row_block(block, carry):
            real_acc, imag_acc = carry
            tile_block = lax.dynamic_index_in_dim(hoppings, block, 0, keepdims=False).astype(jnp.float32)
            destination_rows = lax.dynamic_index_in_dim(block_ids, block, 0, keepdims=False)
            cos_row = lax.dynamic_index_in_dim(cos_weight, block, 0, keepdims=False)
            sin_row = lax.dynamic_index_in_dim(sin_weight, block, 0, keepdims=False)
            real_acc = real_acc.at[destination_rows].add(cos_row[:, None, None] * tile_block)
            imag_acc = imag_acc.at[destination_rows].add(sin_row[:, None, None] * tile_block)
            return (real_acc, imag_acc)

        empty_blocks = jnp.zeros((TORB * TORB, TS, TS), jnp.float32)
        real_acc, imag_acc = lax.fori_loop(0, N_ROWS, add_row_block, (empty_blocks, empty_blocks))
        matrix = jnp.stack([real_acc, imag_acc]).astype(jnp.bfloat16)
        matrix = lax.optimization_barrier(matrix).astype(jnp.float32).reshape(2, TORB, TORB, TS, TS)
        vector_f32 = point_vectors.astype(jnp.float32).reshape(2, TORB, TS, NVEC)
        product = jnp.einsum('pijab,qjbv->piaqv', matrix, vector_f32, precision=lax.Precision.HIGHEST)
        real_part = product[0, :, :, 0] - product[1, :, :, 1]
        imag_part = product[0, :, :, 1] + product[1, :, :, 0]
        return jnp.stack([real_part, imag_part]).reshape(2, TORB * TS, NVEC)

    return lax.map(one_point, (phase_angle, vectors))
```

```python
import functools

import jax
import jax.numpy as jnp
from jax import lax
from jax.experimental import pallas as pl
from jax.experimental.pallas import tpu as pltpu
from jax.sharding import PartitionSpec as P

NLAT = 9
BAND = 16
GROUP = 4
DEPTH = 4
MESH = pl.DeviceIdType.MESH


def spans(total, size):
    return [(start, min(size, total - start)) for start in range(0, total, size)]


def exchange_kernel(group_size, row_shards, hop, meta, vec, all_hop, all_meta, win,
                    hop_own, meta_own, send_sem, recv_sem, local_sem):
    slots = hop.shape[0]
    row_tiles = vec.shape[2]
    ka = lax.axis_index("ka")
    row = lax.axis_index("rows")
    odd = lax.rem(row, 2)
    even = 1 - odd
    sign = 1 - 2 * odd
    partner = ka + 1 - 2 * lax.rem(ka, 2)
    reach = (BAND + row_tiles - 1) // row_tiles
    depth_of = lambda d: min(row_tiles, BAND - (d - 1) * row_tiles)

    def at_row(step):
        return {"ka": ka, "rows": lax.rem(row + step + 2 * row_shards, row_shards)}

    def at_ka(other):
        return {"ka": other, "rows": row}

    across = [lax.rem(ka + 2 * h, group_size) for h in range(1, group_size // 2)]
    others = [lax.rem(ka + h, group_size) for h in range(1, group_size)]
    forwarding = row_tiles <= BAND and row_shards % 2 == 0 and reach >= 2
    peers = [at_ka(o) for o in others]
    if forwarding:
        peers.append(at_row(sign))
    else:
        peers += [at_row(1), at_row(-1)]
    for d in range(2, reach + 1):
        peers += [at_row(d), at_row(-d)]

    barrier = pltpu.get_barrier_semaphore()
    for peer in peers:
        pl.semaphore_signal(barrier, inc=1, device_id=peer, device_id_type=MESH)

    fetch_hop = pltpu.make_async_copy(hop, hop_own, local_sem.at[0])
    fetch_meta = pltpu.make_async_copy(meta, meta_own, local_sem.at[1])
    fetch_hop.start()
    fetch_meta.start()
    pl.semaphore_wait(barrier, len(peers))

    made = []

    def send(src, dst, device):
        n = len(made)
        copy = pltpu.make_async_remote_copy(
            src_ref=src, dst_ref=dst, send_sem=send_sem.at[n], recv_sem=recv_sem.at[n],
            device_id=device, device_id_type=MESH)
        copy.start()
        made.append(copy)
        return copy

    received = set()

    def arrived(copy):
        copy.wait_recv()
        received.add(id(copy))

    def vec_send(tile, count, step):
        send_to = -step * row_tiles + tile + BAND
        return send(vec.at[:, :, pl.ds(tile, count)], win.at[:, :, pl.ds(send_to, count)], at_row(step))

    def vec_pass(source, tile, count, step):
        here = source * row_tiles + tile + BAND
        there = (source - step) * row_tiles + tile + BAND
        return send(win.at[:, :, pl.ds(here, count)], win.at[:, :, pl.ds(there, count)], at_row(step))

    near_parts = []
    if forwarding:
        second = depth_of(2)
        extra = min(second, row_tiles - 2)
        main = row_tiles - extra
        parts = spans(main, 2)
        near_parts.append(vec_send(even * extra + parts[0][0], parts[0][1], sign))
        turned = vec_send(odd * (row_tiles - extra), extra, -2 * sign) if extra else None
    hop_parts = []
    hop_spans = spans(slots, max(1, slots // 12))
    for h, other in enumerate(across):
        for start, count in hop_spans:
            hop_parts.append((ka + 2 * (h + 1), start, count, send(
                hop.at[pl.ds(start, count)], all_hop.at[ka, pl.ds(start, count)], at_ka(other))))
    for other in others:
        send(meta, all_meta.at[ka], at_ka(other))
    if forwarding:
        for start, count in parts[1:]:
            near_parts.append(vec_send(even * extra + start, count, sign))
        if extra:
            vec_send(odd * (row_tiles - extra), extra, sign)
        vec_send(even * (row_tiles - second), second, 2 * sign)
        if second > extra:
            vec_send(even * extra + odd * (row_tiles - second), second - extra, -2 * sign)
    else:
        first = depth_of(1)
        vec_send(0, first, -1)
        vec_send(row_tiles - first, first, 1)
        if reach >= 2:
            vec_send(0, depth_of(2), -2)
            vec_send(row_tiles - depth_of(2), depth_of(2), 2)
    for d in range(3, reach + 1):
        vec_send(0, depth_of(d), -d)
        vec_send(row_tiles - depth_of(d), depth_of(d), d)
    for start, count in hop_spans:
        send(hop.at[pl.ds(start, count)], all_hop.at[ka, pl.ds(start, count)], at_ka(partner))

    fetch_hop.wait()
    fetch_meta.wait()
    store_hop = pltpu.make_async_copy(hop_own, all_hop.at[ka], local_sem.at[0])
    store_meta = pltpu.make_async_copy(meta_own, all_meta.at[ka], local_sem.at[1])
    store_hop.start()
    store_meta.start()

    def pass_hop(n):
        owner, start, count, copy = hop_parts[n]
        owner = lax.rem(owner, group_size)
        arrived(copy)
        block = all_hop.at[owner, pl.ds(start, count)]
        send(block, block, at_ka(partner))

    done = 0
    if forwarding:
        for n, copy in enumerate(near_parts):
            arrived(copy)
            start, count = parts[n]
            vec_pass(sign, odd * extra + start, count, 2 * sign)
            if n == 1 and extra:
                arrived(turned)
                vec_pass(2 * sign, odd * (row_tiles - extra), extra, sign)
            until = len(hop_parts) * (n + 1) // (len(near_parts) + 1)
            while done < until:
                pass_hop(done)
                done += 1
        if len(near_parts) < 2 and extra:
            arrived(turned)
            vec_pass(2 * sign, odd * (row_tiles - extra), extra, sign)
    while done < len(hop_parts):
        pass_hop(done)
        done += 1

    store_hop.wait()
    store_meta.wait()
    for copy in made:
        if id(copy) not in received:
            copy.wait_recv()
    for copy in made:
        copy.wait_send()


def exchange(group_size, row_shards, hop, meta, vec):
    slots = hop.shape[0]
    width = vec.shape[2] + 2 * BAND
    return pl.pallas_call(
        functools.partial(exchange_kernel, group_size, row_shards),
        out_shape=(
            jax.ShapeDtypeStruct((group_size,) + hop.shape, hop.dtype),
            jax.ShapeDtypeStruct((group_size,) + meta.shape, meta.dtype),
            jax.ShapeDtypeStruct(vec.shape[:2] + (width,) + vec.shape[3:], vec.dtype),
        ),
        in_specs=[pl.BlockSpec(memory_space=pl.ANY)] * 3,
        out_specs=(pl.BlockSpec(memory_space=pl.ANY),) * 3,
        scratch_shapes=[
            pltpu.VMEM(hop.shape, hop.dtype),
            pltpu.VMEM(meta.shape, meta.dtype),
            pltpu.SemaphoreType.DMA((96,)),
            pltpu.SemaphoreType.DMA((96,)),
            pltpu.SemaphoreType.DMA((2,)),
        ],
        compiler_params=pltpu.CompilerParams(
            collective_id=0, has_side_effects=True, vmem_limit_bytes=60 * 2**20),
        name="exchange",
    )(hop, meta, vec)


def product_kernel(group_count, order, places, group_rows, coef, hop, vec, win, out,
                   vwin, acc, tiles, mats, tile_sem, vec_sem, out_sem):
    kpoints = vec.shape[0]
    row_tiles = vec.shape[2]
    groups = group_count[0]
    edge = vec.shape[3]

    def tile_copies(g):
        slot = lax.rem(g, DEPTH)
        return [
            pltpu.make_async_copy(hop.at[order[g * GROUP + j]], tiles.at[slot, j], tile_sem.at[slot, j])
            for j in range(GROUP)
        ]

    regions = [
        (win.at[:, :, pl.ds(0, BAND)], vwin.at[:, :, pl.ds(0, BAND)]),
        (vec, vwin.at[:, :, pl.ds(BAND, row_tiles)]),
        (win.at[:, :, pl.ds(BAND + row_tiles, BAND)], vwin.at[:, :, pl.ds(BAND + row_tiles, BAND)]),
    ]
    loads = [pltpu.make_async_copy(s, d, vec_sem.at[n]) for n, (s, d) in enumerate(regions)]
    for copy in loads:
        copy.start()
    for ahead in range(DEPTH - 1):
        @pl.when(ahead < groups)
        def _(ahead=ahead):
            for copy in tile_copies(ahead):
                copy.start()

    def clear(i, _):
        for k in range(kpoints):
            for part in range(2):
                acc[k, part, i] = jnp.zeros(acc.shape[3:], acc.dtype)
        return 0

    lax.fori_loop(0, row_tiles, clear, 0)
    for copy in loads:
        copy.wait()

    def step(g, _):
        @pl.when(g + DEPTH - 1 < groups)
        def _():
            for copy in tile_copies(g + DEPTH - 1):
                copy.start()

        for copy in tile_copies(g):
            copy.wait()
        slot = lax.rem(g, DEPTH)
        target = group_rows[g]
        for k in range(kpoints):
            for j in range(GROUP):
                n = g * GROUP + j
                tile = tiles[slot, j].astype(jnp.float32)
                cosine = (coef[2 * k, n] * tile).astype(jnp.bfloat16)
                sine = coef[2 * k + 1, n] * tile
                left = j * 2 * edge
                mats[k, :edge, left:left + edge] = cosine
                mats[k, edge:, left + edge:left + 2 * edge] = cosine
                mats[k, edge:, left:left + edge] = sine.astype(jnp.bfloat16)
                mats[k, :edge, left + edge:left + 2 * edge] = (-sine).astype(jnp.bfloat16)
        for k in range(kpoints):
            stacked = jnp.concatenate(
                [vwin[k, part, places[g * GROUP + j]] for j in range(GROUP) for part in range(2)],
                axis=0)
            result = jnp.dot(mats[k], stacked, preferred_element_type=jnp.float32)
            for part in range(2):
                acc[k, part, target] += result[part * edge:(part + 1) * edge]
        return 0

    lax.fori_loop(0, groups, step, 0)
    store = pltpu.make_async_copy(acc, out, out_sem)
    store.start()
    store.wait()


def product(group_count, order, places, group_rows, coef, hop, vec, win):
    kpoints, _, row_tiles, edge, vec_count = vec.shape
    smem = pl.BlockSpec(memory_space=pltpu.SMEM)
    return pl.pallas_call(
        product_kernel,
        out_shape=jax.ShapeDtypeStruct(vec.shape, jnp.float32),
        in_specs=[smem] * 5 + [pl.BlockSpec(memory_space=pl.ANY)] * 3,
        out_specs=pl.BlockSpec(memory_space=pl.ANY),
        scratch_shapes=[
            pltpu.VMEM(win.shape, win.dtype),
            pltpu.VMEM(vec.shape, jnp.float32),
            pltpu.VMEM((DEPTH, GROUP, edge, edge), hop.dtype),
            pltpu.VMEM((kpoints, 2 * edge, 2 * GROUP * edge), jnp.bfloat16),
            pltpu.SemaphoreType.DMA((DEPTH, GROUP)),
            pltpu.SemaphoreType.DMA((3,)),
            pltpu.SemaphoreType.DMA,
        ],
        compiler_params=pltpu.CompilerParams(vmem_limit_bytes=60 * 2**20),
        name="product",
    )(group_count, order, places, group_rows, coef, hop, vec, win)


def body(hoppings, tile_rows, tile_cols, tile_lats, tile_counts, phase_angle, vectors):
    edge = hoppings.shape[2]
    per_device = hoppings.shape[1]
    group_size = lax.axis_size("ka")
    row_shards = lax.axis_size("rows")
    kpoints, _, orbitals, vec_count = vectors.shape
    row_tiles = orbitals // edge
    total_tiles = row_tiles * row_shards
    row_start = lax.axis_index("rows") * row_tiles
    slots = group_size * per_device

    lanes = -(-per_device // 128) * 128
    live = lax.broadcasted_iota(jnp.int32, (1, per_device), 1) < tile_counts
    rows = jnp.where(live, tile_rows - row_start, row_tiles)
    place = jnp.mod(tile_cols - row_start + BAND, total_tiles)
    meta = jnp.concatenate([rows, place, tile_lats, jnp.zeros((5, per_device), jnp.int32)], axis=0)
    meta = jnp.pad(meta, ((0, 0), (0, lanes - per_device)))
    vec = vectors.reshape(kpoints, 2, row_tiles, edge, vec_count)
    all_hop, all_meta, win = exchange(group_size, row_shards, hoppings[0], meta, vec)

    all_hop = all_hop.reshape(slots, edge, edge)
    slot_rows = all_meta[:, 0, :per_device].reshape(slots)
    slot_place = all_meta[:, 1, :per_device].reshape(slots)
    slot_lats = all_meta[:, 2, :per_device].reshape(slots)
    group_max = slots // GROUP + row_tiles
    in_row = slot_rows[None, :] == lax.iota(jnp.int32, row_tiles)[:, None]
    row_counts = jnp.sum(in_row.astype(jnp.int32), axis=1)
    row_groups = jnp.maximum((row_counts + GROUP - 1) // GROUP, 1)
    ends = jnp.sum(
        jnp.where(lax.iota(jnp.int32, row_tiles)[None, :] <= lax.iota(jnp.int32, row_tiles)[:, None],
                  row_groups[None, :], 0), axis=1)
    starts = ends - row_groups
    before = lax.iota(jnp.int32, slots)[None, :] < lax.iota(jnp.int32, slots)[:, None]
    same = slot_rows[None, :] == slot_rows[:, None]
    rank = jnp.sum((before & same).astype(jnp.int32), axis=1)
    base = jnp.sum(jnp.where(in_row, starts[:, None], 0), axis=0)
    position = jnp.where(slot_rows < row_tiles, base * GROUP + rank, -1)
    hit = lax.iota(jnp.int32, group_max * GROUP)[:, None] == position[None, :]

    def arranged(values):
        return jnp.sum(jnp.where(hit, values[None, :], 0), axis=1)

    order = arranged(lax.iota(jnp.int32, slots))
    places = arranged(slot_place)
    lats = arranged(slot_lats + 1) - 1
    group_rows = jnp.minimum(
        jnp.sum((lax.iota(jnp.int32, group_max)[:, None] >= ends[None, :]).astype(jnp.int32), axis=1),
        row_tiles - 1)
    weights = jnp.stack([jnp.cos(phase_angle), jnp.sin(phase_angle)], axis=1).reshape(2 * kpoints, -1)
    coef = jnp.sum(
        jnp.where(lats[None, :, None] == lax.iota(jnp.int32, weights.shape[1]), weights[:, None, :], 0.0),
        axis=2)
    out = product(ends[-1:], order, places, group_rows, coef, all_hop, vec, win)
    return out.reshape(kpoints, 2, orbitals, vec_count)


def solution(mesh):
    return jax.shard_map(
        body,
        mesh=mesh,
        in_specs=(
            P("rows", "ka", None, None),
            P("rows", "ka"),
            P("rows", "ka"),
            P("rows", "ka"),
            P("rows", "ka"),
            P("ka", None),
            P("ka", None, "rows", None),
        ),
        out_specs=P("ka", None, "rows", None),
        check_vma=False,
    )
```

```python
import functools

import jax
import jax.numpy as jnp
from jax import lax
from jax.experimental import pallas as pl
from jax.experimental.pallas import tpu as pltpu
from jax.sharding import PartitionSpec as P

NLAT = 9
BAND = 16
GROUP = 4
STAGES = 2
MESH = pl.DeviceIdType.MESH


def spans(total, size):
    return [(start, min(size, total - start)) for start in range(0, total, size)]


def exchange_kernel(group_size, row_shards, hop, meta, vec, all_hop, all_meta, win,
                    send_sem, recv_sem, local_sem):
    slots = hop.shape[0]
    row_tiles = vec.shape[2]
    ka = lax.axis_index("ka")
    row = lax.axis_index("rows")
    odd = lax.rem(row, 2)
    even = 1 - odd
    sign = 1 - 2 * odd
    partner = ka + 1 - 2 * lax.rem(ka, 2)
    reach = (BAND + row_tiles - 1) // row_tiles
    depth_of = lambda d: min(row_tiles, BAND - (d - 1) * row_tiles)

    def at_row(step):
        return {"ka": ka, "rows": lax.rem(row + step + 2 * row_shards, row_shards)}

    def at_ka(other):
        return {"ka": other, "rows": row}

    across = [lax.rem(ka + 2 * h, group_size) for h in range(1, group_size // 2)]
    others = [lax.rem(ka + h, group_size) for h in range(1, group_size)]
    forwarding = row_tiles <= BAND and row_shards % 2 == 0 and reach >= 2
    peers = [at_ka(o) for o in others]
    if forwarding:
        peers.append(at_row(sign))
    else:
        peers += [at_row(1), at_row(-1)]
    for d in range(2, reach + 1):
        peers += [at_row(d), at_row(-d)]

    barrier = pltpu.get_barrier_semaphore()
    for peer in peers:
        pl.semaphore_signal(barrier, inc=1, device_id=peer, device_id_type=MESH)

    local = [
        pltpu.make_async_copy(hop, all_hop.at[pl.ds(ka * slots, slots)], local_sem.at[0]),
        pltpu.make_async_copy(meta, all_meta.at[ka], local_sem.at[1]),
        pltpu.make_async_copy(vec, win.at[:, :, pl.ds(BAND, row_tiles)], local_sem.at[2]),
    ]
    for copy in local:
        copy.start()
    pl.semaphore_wait(barrier, len(peers))

    made = []

    def send(src, dst, device):
        n = len(made)
        copy = pltpu.make_async_remote_copy(
            src_ref=src, dst_ref=dst, send_sem=send_sem.at[n], recv_sem=recv_sem.at[n],
            device_id=device, device_id_type=MESH)
        copy.start()
        made.append(copy)
        return copy

    received = set()

    def arrived(copy):
        copy.wait_recv()
        received.add(id(copy))

    def vec_send(tile, count, step):
        send_to = -step * row_tiles + tile + BAND
        return send(vec.at[:, :, pl.ds(tile, count)], win.at[:, :, pl.ds(send_to, count)], at_row(step))

    def vec_pass(source, tile, count, step):
        here = source * row_tiles + tile + BAND
        there = (source - step) * row_tiles + tile + BAND
        return send(win.at[:, :, pl.ds(here, count)], win.at[:, :, pl.ds(there, count)], at_row(step))

    near_parts = []
    if forwarding:
        second = depth_of(2)
        extra = min(second, row_tiles - 2)
        main = row_tiles - extra
        parts = spans(main, 2)
        near_parts.append(vec_send(even * extra + parts[0][0], parts[0][1], sign))
        turned = vec_send(odd * (row_tiles - extra), extra, -2 * sign) if extra else None
    hop_parts = []
    hop_spans = spans(slots, max(1, slots // 12))
    for h, other in enumerate(across):
        for start, count in hop_spans:
            hop_parts.append((ka + 2 * (h + 1), start, count, send(
                hop.at[pl.ds(start, count)], all_hop.at[pl.ds(ka * slots + start, count)], at_ka(other))))
    for other in others:
        send(meta, all_meta.at[ka], at_ka(other))
    if forwarding:
        for start, count in parts[1:]:
            near_parts.append(vec_send(even * extra + start, count, sign))
        if extra:
            vec_send(odd * (row_tiles - extra), extra, sign)
        vec_send(even * (row_tiles - second), second, 2 * sign)
        if second > extra:
            vec_send(even * extra + odd * (row_tiles - second), second - extra, -2 * sign)
    else:
        first = depth_of(1)
        vec_send(0, first, -1)
        vec_send(row_tiles - first, first, 1)
        if reach >= 2:
            vec_send(0, depth_of(2), -2)
            vec_send(row_tiles - depth_of(2), depth_of(2), 2)
    for d in range(3, reach + 1):
        vec_send(0, depth_of(d), -d)
        vec_send(row_tiles - depth_of(d), depth_of(d), d)
    for start, count in hop_spans:
        send(hop.at[pl.ds(start, count)], all_hop.at[pl.ds(ka * slots + start, count)], at_ka(partner))

    def pass_hop(n):
        owner, start, count, copy = hop_parts[n]
        owner = lax.rem(owner, group_size)
        arrived(copy)
        block = all_hop.at[pl.ds(owner * slots + start, count)]
        send(block, block, at_ka(partner))

    done = 0
    if forwarding:
        for n, copy in enumerate(near_parts):
            arrived(copy)
            start, count = parts[n]
            vec_pass(sign, odd * extra + start, count, 2 * sign)
            if n == 1 and extra:
                arrived(turned)
                vec_pass(2 * sign, odd * (row_tiles - extra), extra, sign)
            until = len(hop_parts) * (n + 1) // (len(near_parts) + 1)
            while done < until:
                pass_hop(done)
                done += 1
        if len(near_parts) < 2 and extra:
            arrived(turned)
            vec_pass(2 * sign, odd * (row_tiles - extra), extra, sign)
    while done < len(hop_parts):
        pass_hop(done)
        done += 1

    for copy in local:
        copy.wait()
    for copy in made:
        if id(copy) not in received:
            copy.wait_recv()
    for copy in made:
        copy.wait_send()


def exchange(group_size, row_shards, hop, meta, vec):
    slots = hop.shape[0]
    width = vec.shape[2] + 2 * BAND
    return pl.pallas_call(
        functools.partial(exchange_kernel, group_size, row_shards),
        out_shape=(
            pltpu.VMEM((group_size * slots,) + hop.shape[1:], hop.dtype),
            jax.ShapeDtypeStruct((group_size,) + meta.shape, meta.dtype),
            pltpu.VMEM(vec.shape[:2] + (width,) + vec.shape[3:], vec.dtype),
        ),
        in_specs=[pl.BlockSpec(memory_space=pl.ANY)] * 3,
        out_specs=(pl.BlockSpec(memory_space=pltpu.VMEM), pl.BlockSpec(memory_space=pl.ANY),
                   pl.BlockSpec(memory_space=pltpu.VMEM)),
        scratch_shapes=[
            pltpu.SemaphoreType.DMA((96,)),
            pltpu.SemaphoreType.DMA((96,)),
            pltpu.SemaphoreType.DMA((3,)),
        ],
        compiler_params=pltpu.CompilerParams(
            collective_id=0, has_side_effects=True, vmem_limit_bytes=2**20),
        name="exchange",
    )(pltpu.with_memory_space_constraint(hop, pltpu.HBM), meta,
      pltpu.with_memory_space_constraint(vec, pltpu.HBM))


def bits_of(count):
    return max(1, (count - 1).bit_length())


def arrange(meta, bucket, counts, group_size, per_device):
    slots = group_size * per_device
    buckets = counts.shape[0]
    for row in range(buckets):
        counts[row] = 0

    def take(i, _):
        for owner in range(group_size):
            row = meta[owner, 0, i]
            held = counts[row]
            bucket[row * (slots + GROUP) + held] = meta[owner, 1, i]
            counts[row] = held + 1
        return 0

    lax.fori_loop(0, per_device, take, 0, unroll=8 if per_device % 8 == 0 else 1)


def multiply(rows, group_stride, place_bits, tile_bits, pad, bucket, counts, weights, tiles, vwin, accs):
    kpoints = vwin.shape[0]

    def each_row(row, finish):
        held = counts[row]
        base = row * group_stride
        for j in range(GROUP - 1):
            bucket[base + held + j] = pad

        def step(g, _):
            for j in range(GROUP):
                code = bucket[base + g * GROUP + j]
                index = code & (2**tile_bits - 1)
                place = (code >> tile_bits) & (2**place_bits - 1)
                lattice = code >> (tile_bits + place_bits)
                tile = tiles[index].astype(jnp.float32)
                for k in range(kpoints):
                    stacked = jnp.concatenate([vwin[k, 0, place], vwin[k, 1, place]], axis=0)
                    pltpu.matmul_push_rhs(stacked, staging_register=j % 2, mxu_index=k % 2)
                    cosine = (weights[2 * k, lattice] * tile).astype(jnp.bfloat16)
                    sine = (weights[2 * k + 1, lattice] * tile).astype(jnp.bfloat16)
                    matrix = jnp.concatenate(
                        [jnp.concatenate([cosine, -sine], axis=1),
                         jnp.concatenate([sine, cosine], axis=1)], axis=0)
                    pltpu.matmul_acc_lhs(accs[k], matrix, load_staged_rhs=j % 2)
            return 0

        lax.fori_loop(0, (held + GROUP - 1) // GROUP, step, 0)
        finish(row)

    return each_row


def product_kernel(group_size, per_device, tile_bits, place_bits, pad, meta, weights, tiles, vwin, out,
                   bucket, counts, stage, out_sem):
    kpoints, _, _, edge, _ = vwin.shape
    row_tiles = out.shape[2]
    arrange(meta, bucket, counts, group_size, per_device)

    def run(*accs):
        def store(row):
            slot = lax.rem(row, STAGES)
            return pltpu.make_async_copy(stage.at[slot], out.at[:, :, row], out_sem.at[slot])

        def finish(row):
            @pl.when(row >= STAGES)
            def _():
                store(row - STAGES).wait()

            slot = lax.rem(row, STAGES)
            for k in range(kpoints):
                result = pltpu.matmul_pop(accs[k])
                for part in range(2):
                    stage[slot, k, part] = result[part * edge:(part + 1) * edge]
            store(row).start()

        each_row = multiply(row_tiles, group_size * per_device + GROUP, place_bits, tile_bits, pad, bucket, counts,
                            weights, tiles, vwin, accs)

        def one(row, _):
            each_row(row, finish)
            return 0

        lax.fori_loop(0, row_tiles, one, 0)
        for row in range(max(0, row_tiles - STAGES), row_tiles):
            store(row).wait()

    pl.run_scoped(run, *[pltpu.ACC(k % 2)((2 * edge, vwin.shape[4]), jnp.float32) for k in range(kpoints)])


def product(per_device, tile_bits, place_bits, pad, meta, weights, hop, win, row_tiles):
    kpoints, _, _, edge, vec_count = win.shape
    group_size = hop.shape[0] // per_device
    smem = pl.BlockSpec(memory_space=pltpu.SMEM)
    vmem = pl.BlockSpec(memory_space=pltpu.VMEM)
    return pl.pallas_call(
        functools.partial(product_kernel, group_size, per_device, tile_bits, place_bits, pad),
        out_shape=jax.ShapeDtypeStruct((kpoints, 2, row_tiles, edge, vec_count), jnp.float32),
        in_specs=[smem] * 2 + [vmem] * 2,
        out_specs=pl.BlockSpec(memory_space=pl.ANY),
        scratch_shapes=[
            pltpu.SMEM(((row_tiles + 1) * (hop.shape[0] + GROUP),), jnp.int32),
            pltpu.SMEM((row_tiles + 1,), jnp.int32),
            pltpu.VMEM((STAGES, kpoints, 2, edge, vec_count), jnp.float32),
            pltpu.SemaphoreType.DMA((STAGES,)),
        ],
        compiler_params=pltpu.CompilerParams(vmem_limit_bytes=12 * 2**20),
        name="product",
    )(meta, weights,
      pltpu.with_memory_space_constraint(hop, pltpu.VMEM),
      pltpu.with_memory_space_constraint(win, pltpu.VMEM))


def body(hoppings, tile_rows, tile_cols, tile_lats, tile_counts, phase_angle, vectors):
    edge = hoppings.shape[2]
    per_device = hoppings.shape[1]
    group_size = lax.axis_size("ka")
    row_shards = lax.axis_size("rows")
    kpoints, _, orbitals, vec_count = vectors.shape
    lattices = phase_angle.shape[1]
    row_tiles = orbitals // edge
    total_tiles = row_tiles * row_shards
    row_start = lax.axis_index("rows") * row_tiles
    slots = group_size * per_device
    tile_bits = bits_of(slots)
    place_bits = bits_of(row_tiles + 2 * BAND)

    lanes = -(-per_device // 128) * 128
    slot = lax.broadcasted_iota(jnp.int32, (1, per_device), 1)
    rows = jnp.where(slot < tile_counts, tile_rows - row_start, row_tiles)
    place = jnp.mod(tile_cols - row_start + BAND, total_tiles)
    code = (((tile_lats << place_bits) + place) << tile_bits) + lax.axis_index("ka") * per_device + slot
    meta = jnp.concatenate([rows, code, jnp.zeros((6, per_device), jnp.int32)], axis=0)
    meta = jnp.pad(meta, ((0, 0), (0, lanes - per_device)))
    vec = vectors.reshape(kpoints, 2, row_tiles, edge, vec_count)
    weights = jnp.stack([jnp.cos(phase_angle), jnp.sin(phase_angle)], axis=1).reshape(2 * kpoints, lattices)
    weights = jnp.pad(weights, ((0, 0), (0, 1)))
    all_hop, all_meta, win = exchange(group_size, row_shards, hoppings[0], meta, vec)
    pad = lattices << (place_bits + tile_bits)
    out = product(per_device, tile_bits, place_bits, pad, all_meta, weights, all_hop, win, row_tiles)
    return out.reshape(kpoints, 2, orbitals, vec_count)


def solution(mesh):
    return jax.shard_map(
        body,
        mesh=mesh,
        in_specs=(
            P("rows", "ka", None, None),
            P("rows", "ka"),
            P("rows", "ka"),
            P("rows", "ka"),
            P("rows", "ka"),
            P("ka", None),
            P("ka", None, "rows", None),
        ),
        out_specs=P("ka", None, "rows", None),
        check_vma=False,
    )
```

```python
import functools

import jax
import jax.numpy as jnp
from jax import lax
from jax.experimental import pallas as pl
from jax.experimental.pallas import tpu as pltpu
from jax.sharding import PartitionSpec as P

NLAT = 9
BAND = 16
GROUP = 4
LATE_GROUP = 2
MESH = pl.DeviceIdType.MESH


def spans(total, size):
    return [(start, min(size, total - start)) for start in range(0, total, size)]


def late_tiles(row_tiles, row_shards):
    reach = (BAND + row_tiles - 1) // row_tiles
    if row_tiles > BAND or row_shards % 2 or reach < 2:
        return 0, 0
    extra = min(row_tiles, BAND - row_tiles, row_tiles - 2)
    return min(extra, row_tiles - extra), extra


def exchange_kernel(group_size, row_shards, hop, meta, vec, all_hop, all_meta, win, *rest):
    across_tiles, beside_tiles = late_tiles(vec.shape[2], row_shards)
    if across_tiles and beside_tiles:
        across_out, beside_out, send_sem, recv_sem, local_sem = rest
    else:
        send_sem, recv_sem, local_sem = rest

    slots = hop.shape[0]
    row_tiles = vec.shape[2]
    ka = lax.axis_index("ka")
    row = lax.axis_index("rows")
    odd = lax.rem(row, 2)
    even = 1 - odd
    sign = 1 - 2 * odd
    partner = ka + 1 - 2 * lax.rem(ka, 2)
    reach = (BAND + row_tiles - 1) // row_tiles
    depth_of = lambda d: min(row_tiles, BAND - (d - 1) * row_tiles)

    def at_row(step):
        return {"ka": ka, "rows": lax.rem(row + step + 2 * row_shards, row_shards)}

    def at_ka(other):
        return {"ka": other, "rows": row}

    across = [lax.rem(ka + 2 * h, group_size) for h in range(1, group_size // 2)]
    others = [lax.rem(ka + h, group_size) for h in range(1, group_size)]
    forwarding = row_tiles <= BAND and row_shards % 2 == 0 and reach >= 2
    peers = [at_ka(o) for o in others]
    if forwarding:
        peers.append(at_row(sign))
    else:
        peers += [at_row(1), at_row(-1)]
    for d in range(2, reach + 1):
        peers += [at_row(d), at_row(-d)]

    barrier = pltpu.get_barrier_semaphore()
    for peer in peers:
        pl.semaphore_signal(barrier, inc=1, device_id=peer, device_id_type=MESH)

    local = [
        pltpu.make_async_copy(hop, all_hop.at[pl.ds(ka * slots, slots)], local_sem.at[0]),
        pltpu.make_async_copy(meta, all_meta.at[ka], local_sem.at[1]),
        pltpu.make_async_copy(vec, win.at[:, :, pl.ds(BAND, row_tiles)], local_sem.at[2]),
    ]
    for copy in local:
        copy.start()
    pl.semaphore_wait(barrier, len(peers))

    made = []

    def send(src, dst, device):
        n = len(made)
        copy = pltpu.make_async_remote_copy(
            src_ref=src, dst_ref=dst, send_sem=send_sem.at[n], recv_sem=recv_sem.at[n],
            device_id=device, device_id_type=MESH)
        copy.start()
        made.append(copy)
        return copy

    received = set()

    def arrived(copy):
        copy.wait_recv()
        received.add(id(copy))

    def vec_send(tile, count, step):
        send_to = -step * row_tiles + tile + BAND
        return send(vec.at[:, :, pl.ds(tile, count)], win.at[:, :, pl.ds(send_to, count)], at_row(step))

    def vec_pass(source, tile, count, step):
        here = source * row_tiles + tile + BAND
        there = (source - step) * row_tiles + tile + BAND
        return send(win.at[:, :, pl.ds(here, count)], win.at[:, :, pl.ds(there, count)], at_row(step))

    near_parts = []
    if forwarding:
        second = depth_of(2)
        extra = min(second, row_tiles - 2)
        main = row_tiles - extra
        kept = main - across_tiles
        parts = spans(kept, 2) + [(kept + start, count) for start, count in spans(across_tiles, 2)]

        def part_tile(parity_even, parity_odd, start, count):
            return parity_even * (extra + start) + parity_odd * (main - start - count)

        near_parts.append(vec_send(part_tile(even, odd, *parts[0]), parts[0][1], sign))
        turned = vec_send(odd * (row_tiles - extra), extra, -2 * sign) if extra else None
    hop_parts = []
    hop_spans = spans(slots, max(1, slots // 12))
    for h, other in enumerate(across):
        for start, count in hop_spans:
            hop_parts.append((ka + 2 * (h + 1), start, count, send(
                hop.at[pl.ds(start, count)], all_hop.at[pl.ds(ka * slots + start, count)], at_ka(other))))
    for other in others:
        send(meta, all_meta.at[ka], at_ka(other))
    if forwarding:
        for start, count in parts[1:]:
            near_parts.append(vec_send(part_tile(even, odd, start, count), count, sign))
        if extra and not beside_tiles:
            vec_send(odd * (row_tiles - extra), extra, sign)
        vec_send(even * (row_tiles - second), second, 2 * sign)
        if second > extra:
            vec_send(even * extra + odd * (row_tiles - second), second - extra, -2 * sign)
    else:
        first = depth_of(1)
        vec_send(0, first, -1)
        vec_send(row_tiles - first, first, 1)
        if reach >= 2:
            vec_send(0, depth_of(2), -2)
            vec_send(row_tiles - depth_of(2), depth_of(2), 2)
    for d in range(3, reach + 1):
        vec_send(0, depth_of(d), -d)
        vec_send(row_tiles - depth_of(d), depth_of(d), d)
    for start, count in hop_spans:
        send(hop.at[pl.ds(start, count)], all_hop.at[pl.ds(ka * slots + start, count)], at_ka(partner))

    def pass_hop(n):
        owner, start, count, copy = hop_parts[n]
        owner = lax.rem(owner, group_size)
        arrived(copy)
        block = all_hop.at[pl.ds(owner * slots + start, count)]
        send(block, block, at_ka(partner))

    if beside_tiles:
        local[2].wait()
        hold = pltpu.make_async_copy(
            win.at[:, :, pl.ds(BAND + odd * (row_tiles - beside_tiles), beside_tiles)], beside_out, local_sem.at[3])
        hold.start()
        local[2] = hold

    done = 0
    if forwarding:
        for n, copy in enumerate(near_parts):
            arrived(copy)
            start, count = parts[n]
            tile = part_tile(odd, even, start, count)
            if start < kept:
                vec_pass(sign, tile, count, 2 * sign)
            else:
                first = part_tile(odd, even, kept, across_tiles)
                hold = pltpu.make_async_copy(
                    win.at[:, :, pl.ds(sign * row_tiles + tile + BAND, count)],
                    across_out.at[:, :, pl.ds(tile - first, count)], local_sem.at[4 + n])
                hold.start()
                local.append(hold)
            if n == 1 and extra:
                arrived(turned)
                vec_pass(2 * sign, odd * (row_tiles - extra), extra, sign)
            until = len(hop_parts) * (n + 1) // (len(near_parts) + 1)
            while done < until:
                pass_hop(done)
                done += 1
        if len(near_parts) < 2 and extra:
            arrived(turned)
            vec_pass(2 * sign, odd * (row_tiles - extra), extra, sign)
    while done < len(hop_parts):
        pass_hop(done)
        done += 1

    for copy in local:
        copy.wait()
    for copy in made:
        if id(copy) not in received:
            copy.wait_recv()
    for copy in made:
        copy.wait_send()


def exchange(group_size, row_shards, hop, meta, vec):
    slots = hop.shape[0]
    width = vec.shape[2] + 2 * BAND
    late = tuple(
        jax.ShapeDtypeStruct(vec.shape[:2] + (count,) + vec.shape[3:], vec.dtype)
        for count in late_tiles(vec.shape[2], row_shards) if count)
    return pl.pallas_call(
        functools.partial(exchange_kernel, group_size, row_shards),
        out_shape=(
            pltpu.VMEM((group_size * slots,) + hop.shape[1:], hop.dtype),
            jax.ShapeDtypeStruct((group_size,) + meta.shape, meta.dtype),
            pltpu.VMEM(vec.shape[:2] + (width,) + vec.shape[3:], vec.dtype),
        ) + late,
        in_specs=[pl.BlockSpec(memory_space=pl.ANY)] * 3,
        out_specs=(pl.BlockSpec(memory_space=pltpu.VMEM), pl.BlockSpec(memory_space=pl.ANY),
                   pl.BlockSpec(memory_space=pltpu.VMEM)) + (pl.BlockSpec(memory_space=pl.ANY),) * len(late),
        scratch_shapes=[
            pltpu.SemaphoreType.DMA((96,)),
            pltpu.SemaphoreType.DMA((96,)),
            pltpu.SemaphoreType.DMA((16,)),
        ],
        compiler_params=pltpu.CompilerParams(
            collective_id=0, has_side_effects=True, vmem_limit_bytes=2**20),
        name="exchange",
    )(pltpu.with_memory_space_constraint(hop, pltpu.HBM), meta,
      pltpu.with_memory_space_constraint(vec, pltpu.HBM))


def bits_of(count):
    return max(1, (count - 1).bit_length())


def arrange(meta, bucket, counts, group_size, per_device):
    stride = group_size * per_device + GROUP
    for row in range(counts.shape[0]):
        counts[row] = 0

    def take(i, _):
        for owner in range(group_size):
            row = meta[owner, 0, i]
            held = counts[row]
            bucket[row * stride + held] = meta[owner, 1, i]
            counts[row] = held + 1
        return 0

    lax.fori_loop(0, per_device, take, 0, unroll=8 if per_device % 8 == 0 else 1)


def matrix_of(weights, tile, lattice, k):
    cosine = (weights[2 * k, lattice] * tile).astype(jnp.bfloat16)
    sine = (weights[2 * k + 1, lattice] * tile).astype(jnp.bfloat16)
    return jnp.concatenate(
        [jnp.concatenate([cosine, -sine], axis=1), jnp.concatenate([sine, cosine], axis=1)], axis=0)


def unpacked(bits, code):
    tile_bits, place_bits = bits
    return (code & (2**tile_bits - 1), (code >> tile_bits) & (2**place_bits - 1),
            code >> (tile_bits + place_bits))


def push(bits, code, windows, kpoints, register):
    _, place, _ = unpacked(bits, code)
    for k in range(kpoints):
        if len(windows) == 1:
            parts = [windows[0][k, part, place] for part in range(2)]
        else:
            split = windows[0].shape[2]
            near, far = jnp.minimum(place, split - 1), jnp.maximum(place - split, 0)
            parts = [jnp.where(place < split, windows[0][k, part, near], windows[1][k, part, far])
                     for part in range(2)]
        pltpu.matmul_push_rhs(jnp.concatenate(parts, axis=0), staging_register=register, mxu_index=k % 2)


def group(bits, size, at, following, bucket, weights, tiles, windows, accs):
    codes = [bucket[at + j] for j in range(size)]
    for j, code in enumerate(codes):
        push(bits, codes[j + 1] if j + 1 < size else bucket[following], windows, len(accs), (j + 1) % 2)
        index, _, lattice = unpacked(bits, code)
        tile = tiles[index].astype(jnp.float32)
        for k, acc in enumerate(accs):
            pltpu.matmul_acc_lhs(acc, matrix_of(weights, tile, lattice, k), load_staged_rhs=j % 2)


def every_row(bits, size, row_tiles, first, stride, bucket, counts, weights, tiles, windows, accs, spare, finish, done=None):
    kpoints = windows[0].shape[0]
    sets = (accs[:kpoints], accs[kpoints:])

    def one(row, now, before):
        base = (first + row) * stride
        groups = jnp.maximum((counts[first + row] + size - 1) // size, 1)
        after = jnp.minimum(row + 1, row_tiles - 1)

        def follow(g):
            return jnp.where(g + 1 < groups, base + (g + 1) * size, (first + after) * stride)

        group(bits, size, base, follow(0), bucket, weights, tiles, windows, now)
        finish(jnp.maximum(row - 1, 0), [pltpu.matmul_pop(acc) for acc in before])
        if done is not None:
            @pl.when(row > 0)
            def _():
                done(row - 1)

        def step(g, _):
            group(bits, size, base + g * size, follow(g), bucket, weights, tiles, windows, now)
            return 0

        lax.fori_loop(1, groups, step, 0)

    def pair(i, _):
        one(2 * i, sets[0], sets[1])
        one(2 * i + 1, sets[1], sets[0])
        return 0

    push(bits, bucket[first * stride], windows, kpoints, 0)
    lax.fori_loop(0, row_tiles // 2, pair, 0)
    if row_tiles % 2:
        one(row_tiles - 1, sets[0], sets[1])
    finish(row_tiles - 1, [pltpu.matmul_pop(acc) for acc in sets[1 - row_tiles % 2]])
    if done is not None:
        done(row_tiles - 1)
    nothing = jnp.zeros((spare[0].shape[0], 256), jnp.bfloat16)
    for acc in spare:
        pltpu.matmul_acc_lhs(acc, nothing, load_staged_rhs=0)
        pltpu.matmul_pop(acc)


def accumulators(kpoints, edge, vec_count):
    return ([pltpu.ACC(k % 2)((2 * edge, vec_count), jnp.float32) for k in range(kpoints)] * 2
            + [pltpu.ACC(k % 2)((16, vec_count), jnp.float32) for k in range(kpoints)])


def first_kernel(group_size, per_device, row_tiles, bits, pad, meta, weights, tiles, window, total, bucket, counts):
    kpoints, _, _, edge, vec_count = window.shape
    stride = group_size * per_device + GROUP
    arrange(meta, bucket, counts, group_size, per_device)
    for row in range(2 * row_tiles):
        for j in range(GROUP):
            bucket[row * stride + counts[row] + j] = pad

    def run(*accs):
        def finish(row, results):
            for k, result in enumerate(results):
                for part in range(2):
                    total[k, part, row] = result[part * edge:(part + 1) * edge]

        every_row(bits, GROUP, row_tiles, 0, stride, bucket, counts, weights, tiles, [window], accs[:-kpoints],
                  accs[-kpoints:], finish)

    pl.run_scoped(run, *accumulators(kpoints, edge, vec_count))


def second_kernel(stride, bits, bucket, counts, weights, tiles, total, across, beside, out, stage, out_sem):
    kpoints, _, row_tiles, edge, vec_count = total.shape

    def store(row):
        return pltpu.make_async_copy(stage.at[:, :, row], out.at[:, :, row], out_sem.at[row])

    def run(*accs):
        def finish(row, results):
            for k, result in enumerate(results):
                for part in range(2):
                    stage[k, part, row] = total[k, part, row] + result[part * edge:(part + 1) * edge]

        every_row(bits, LATE_GROUP, row_tiles, row_tiles, stride, bucket, counts, weights, tiles, [across, beside],
                  accs[:-kpoints], accs[-kpoints:], finish, lambda row: store(row).start())

    pl.run_scoped(run, *accumulators(kpoints, edge, vec_count))
    for row in range(row_tiles):
        store(row).wait()


def in_vmem(x):
    return pltpu.with_memory_space_constraint(x, pltpu.VMEM)


SMEM = pl.BlockSpec(memory_space=pltpu.SMEM)
VMEM = pl.BlockSpec(memory_space=pltpu.VMEM)
ANY = pl.BlockSpec(memory_space=pl.ANY)


def first_product(per_device, row_tiles, bits, pad, meta, weights, hop, win):
    kpoints, _, _, edge, vec_count = win.shape
    slots = hop.shape[0]
    buckets = 2 * row_tiles + 1
    work = slots * kpoints * 8 * edge * edge * vec_count
    return pl.pallas_call(
        functools.partial(first_kernel, slots // per_device, per_device, row_tiles, bits, pad),
        out_shape=(
            pltpu.VMEM((kpoints, 2, row_tiles, edge, vec_count), jnp.float32),
            jax.ShapeDtypeStruct((buckets * (slots + GROUP),), jnp.int32),
            jax.ShapeDtypeStruct((buckets,), jnp.int32),
        ),
        in_specs=[SMEM] * 2 + [VMEM] * 2,
        out_specs=(VMEM, SMEM, SMEM),
        compiler_params=pltpu.CompilerParams(vmem_limit_bytes=2**20),
        cost_estimate=pl.CostEstimate(flops=work, bytes_accessed=2**24, transcendentals=0),
        name="first",
    )(meta, weights, in_vmem(hop), in_vmem(win))


def second_product(bits, bucket, counts, weights, hop, total, across, beside):
    kpoints, _, row_tiles, edge, vec_count = total.shape
    return pl.pallas_call(
        functools.partial(second_kernel, hop.shape[0] + GROUP, bits),
        out_shape=jax.ShapeDtypeStruct(total.shape, jnp.float32),
        in_specs=[SMEM] * 3 + [VMEM] * 4,
        out_specs=ANY,
        scratch_shapes=[
            pltpu.VMEM(total.shape, jnp.float32),
            pltpu.SemaphoreType.DMA((row_tiles,)),
        ],
        compiler_params=pltpu.CompilerParams(vmem_limit_bytes=12 * 2**20),
        name="second",
    )(bucket, counts, weights, in_vmem(hop), in_vmem(total), in_vmem(across), in_vmem(beside))


def body(hoppings, tile_rows, tile_cols, tile_lats, tile_counts, phase_angle, vectors):
    edge = hoppings.shape[2]
    per_device = hoppings.shape[1]
    group_size = lax.axis_size("ka")
    row_shards = lax.axis_size("rows")
    kpoints, _, orbitals, vec_count = vectors.shape
    lattices = phase_angle.shape[1]
    row_tiles = orbitals // edge
    total_tiles = row_tiles * row_shards
    shard = lax.axis_index("rows")
    row_start = shard * row_tiles
    across_tiles, beside_tiles = late_tiles(row_tiles, row_shards)
    bits = (bits_of(group_size * per_device), bits_of(row_tiles + 2 * BAND))

    lanes = -(-per_device // 128) * 128
    slot = lax.broadcasted_iota(jnp.int32, (1, per_device), 1)
    place = jnp.mod(tile_cols - row_start + BAND, total_tiles)
    low, high = BAND - row_tiles, BAND + 2 * row_tiles
    even = lax.rem(shard, 2) == 0
    across_at = place - jnp.where(even, low, high - across_tiles)
    beside_at = place - jnp.where(even, high - beside_tiles, low)
    from_across = (across_at >= 0) & (across_at < across_tiles)
    from_beside = (beside_at >= 0) & (beside_at < beside_tiles)
    rows = tile_rows - row_start + jnp.where(from_across | from_beside, row_tiles, 0)
    rows = jnp.where(slot < tile_counts, rows, 2 * row_tiles)
    place = jnp.where(from_across, across_at, jnp.where(from_beside, across_tiles + beside_at, place))
    code = (((tile_lats << bits[1]) + place) << bits[0]) + lax.axis_index("ka") * per_device + slot
    meta = jnp.concatenate([rows, code, jnp.zeros((6, per_device), jnp.int32)], axis=0)
    meta = jnp.pad(meta, ((0, 0), (0, lanes - per_device)))
    vec = vectors.reshape(kpoints, 2, row_tiles, edge, vec_count)
    weights = jnp.stack([jnp.cos(phase_angle), jnp.sin(phase_angle)], axis=1).reshape(2 * kpoints, lattices)
    weights = jnp.pad(weights, ((0, 0), (0, 1)))
    pad = lattices << (bits[0] + bits[1])

    all_hop, all_meta, win, *late = exchange(group_size, row_shards, hoppings[0], meta, vec)
    if late:
        sign = [1 - 2 * (r % 2) for r in range(row_shards)]
        across = lax.ppermute(late[0], "rows", [(r, (r + 2 * sign[r]) % row_shards) for r in range(row_shards)])
        beside = lax.ppermute(late[1], "rows", [(r, r + sign[r]) for r in range(row_shards)])
    total, bucket, counts = first_product(per_device, row_tiles, bits, pad, all_meta, weights, all_hop, win)
    if late:
        total = second_product(bits, bucket, counts, weights, all_hop, total, across, beside)
    return total.reshape(kpoints, 2, orbitals, vec_count)


def solution(mesh):
    return jax.shard_map(
        body,
        mesh=mesh,
        in_specs=(
            P("rows", "ka", None, None),
            P("rows", "ka"),
            P("rows", "ka"),
            P("rows", "ka"),
            P("rows", "ka"),
            P("ka", None),
            P("ka", None, "rows", None),
        ),
        out_specs=P("ka", None, "rows", None),
        check_vma=False,
    )
```

```python
import functools

import jax
import jax.numpy as jnp
from jax import lax
from jax.experimental import pallas as pl
from jax.experimental.pallas import tpu as pltpu
from jax.sharding import PartitionSpec as P

NLAT = 9
BAND = 16
GROUP = 4
LATE_GROUP = 2
MESH = pl.DeviceIdType.MESH


def spans(total, size):
    return [(start, min(size, total - start)) for start in range(0, total, size)]


def late_tiles(row_tiles, row_shards):
    reach = (BAND + row_tiles - 1) // row_tiles
    if row_tiles > BAND or row_shards % 2 or reach < 2:
        return 0, 0
    extra = min(row_tiles, BAND - row_tiles, row_tiles - 2)
    return min(extra, row_tiles - extra), extra


def column(row):
    size = row.shape[1]
    same = (lax.broadcasted_iota(jnp.int32, (size, size), 0) == lax.broadcasted_iota(jnp.int32, (size, size), 1))
    return jnp.sum(jnp.where(same, jnp.broadcast_to(row, (size, size)), 0.0), axis=1, keepdims=True)


def make_plan(row_shards, row_tiles, bits, ints, lives, plan):
    group_size, _, _, per_device = ints.shape
    across_tiles, beside_tiles = late_tiles(row_tiles, row_shards)
    shard = lax.axis_index("rows")
    row_start = shard * row_tiles
    total_tiles = row_tiles * row_shards
    odd = lax.rem(shard, 2)
    even = 1 - odd
    low, high = BAND - row_tiles, BAND + 2 * row_tiles
    across_from = even * low + odd * (high - across_tiles)
    beside_from = even * (high - beside_tiles) + odd * low
    lane = lax.broadcasted_iota(jnp.int32, (1, per_device), 1)

    rows, codes, row_cols, code_cols = [], [], [], []
    for owner in range(group_size):
        place = ints[owner, 1] - row_start + BAND
        place = jnp.where(place < 0, place + total_tiles, place)
        place = jnp.where(place >= total_tiles, place - total_tiles, place)
        row = ints[owner, 0] - row_start
        for begin, count, shift in ((across_from, across_tiles, 0), (beside_from, beside_tiles, across_tiles)):
            if count:
                late = (place >= begin) & (place < begin + count) & (row < row_tiles)
                row = jnp.where(late, row + row_tiles, row)
                place = jnp.where(late, place - begin + shift, place)
        row = jnp.where(lane < lives[owner], row, 2 * row_tiles)
        code = (((ints[owner, 2] + 1) << bits[1]) + place << bits[0]) + owner * per_device + lane
        rows.append(row.astype(jnp.float32))
        codes.append(code.astype(jnp.float32))
        row_cols.append(column(rows[-1]))
        code_cols.append(column(codes[-1]))
    row_col = jnp.concatenate(row_cols, axis=0)
    code_col = jnp.concatenate(code_cols, axis=0)
    slots = group_size * per_device
    buckets = -(-(2 * row_tiles + 1) // 8) * 8
    bucket = lax.broadcasted_iota(jnp.int32, (buckets, 1), 0).astype(jnp.float32)
    held = jnp.zeros((buckets, 1), jnp.float32)
    for row in rows:
        held += jnp.sum(jnp.where(bucket == row, 1.0, 0.0), axis=1, keepdims=True)
    held = jnp.maximum(held, 1.0)
    held = jnp.where(bucket < row_tiles, jnp.floor((held + (GROUP - 1)) * (1 / GROUP)) * GROUP,
                     jnp.floor((held + (LATE_GROUP - 1)) * (1 / LATE_GROUP)) * LATE_GROUP)
    index = lax.broadcasted_iota(jnp.int32, (slots, 1), 0)
    spots = []
    for owner, row in enumerate(rows):
        ahead = (row_col == row) & (index < lane + owner * per_device)
        rank = jnp.sum(jnp.where(ahead, 1.0, 0.0), axis=0, keepdims=True)
        base = jnp.sum(jnp.where(bucket < row, held, 0.0), axis=0, keepdims=True)
        spots.append(column(jnp.where(row < 2 * row_tiles, base + rank, -1.0)))
    spot = jnp.concatenate(spots, axis=0)
    wide = lax.broadcasted_iota(jnp.int32, (1, 128), 1)
    for block in range(plan.shape[0] - 1):
        here = spot == (wide + block * 128).astype(jnp.float32)
        plan[block:block + 1] = jnp.sum(jnp.where(here, code_col, 0.0), axis=0, keepdims=True).astype(jnp.int32)
    starts = jnp.sum(jnp.where(bucket < wide.astype(jnp.float32), held, 0.0), axis=0, keepdims=True)
    plan[plan.shape[0] - 1:] = starts.astype(jnp.int32)


def exchange_kernel(group_size, row_shards, bits, hop, tile_rows, tile_cols, tile_lats, tile_counts, vec,
                    all_hop, plan, win, *rest):
    across_tiles, beside_tiles = late_tiles(vec.shape[2], row_shards)
    if across_tiles and beside_tiles:
        across_out, beside_out, ints, lives, own_lives, send_sem, recv_sem, local_sem = rest
    else:
        ints, lives, own_lives, send_sem, recv_sem, local_sem = rest

    slots = hop.shape[0]
    row_tiles = vec.shape[2]
    own_lives[...] = jnp.full(own_lives.shape, tile_counts[0, 0], jnp.int32)
    ka = lax.axis_index("ka")
    row = lax.axis_index("rows")
    odd = lax.rem(row, 2)
    even = 1 - odd
    sign = 1 - 2 * odd
    partner = ka + 1 - 2 * lax.rem(ka, 2)
    reach = (BAND + row_tiles - 1) // row_tiles
    depth_of = lambda d: min(row_tiles, BAND - (d - 1) * row_tiles)

    def at_row(step):
        return {"ka": ka, "rows": lax.rem(row + step + 2 * row_shards, row_shards)}

    def at_ka(other):
        return {"ka": other, "rows": row}

    across = [lax.rem(ka + 2 * h, group_size) for h in range(1, group_size // 2)]
    others = [lax.rem(ka + h, group_size) for h in range(1, group_size)]
    forwarding = row_tiles <= BAND and row_shards % 2 == 0 and reach >= 2
    peers = [at_ka(o) for o in others]
    if forwarding:
        peers.append(at_row(sign))
    else:
        peers += [at_row(1), at_row(-1)]
    for d in range(2, reach + 1):
        peers += [at_row(d), at_row(-d)]

    barrier = pltpu.get_barrier_semaphore()
    for peer in peers:
        pl.semaphore_signal(barrier, inc=1, device_id=peer, device_id_type=MESH)

    local = [
        pltpu.make_async_copy(hop, all_hop.at[pl.ds(ka * slots, slots)], local_sem.at[0]),
        pltpu.make_async_copy(own_lives, lives.at[ka], local_sem.at[1]),
        pltpu.make_async_copy(vec, win.at[:, :, pl.ds(BAND, row_tiles)], local_sem.at[2]),
    ]
    for field, source in enumerate((tile_rows, tile_cols, tile_lats)):
        local.append(pltpu.make_async_copy(source, ints.at[ka, field], local_sem.at[4 + field]))
    for copy in [local[0]] + local[2:]:
        copy.start()
    pl.semaphore_wait(barrier, len(peers))
    local[1].start()

    made = []

    def send(src, dst, device):
        n = len(made)
        copy = pltpu.make_async_remote_copy(
            src_ref=src, dst_ref=dst, send_sem=send_sem.at[n], recv_sem=recv_sem.at[n],
            device_id=device, device_id_type=MESH)
        copy.start()
        made.append(copy)
        return copy

    received = set()

    def arrived(copy):
        copy.wait_recv()
        received.add(id(copy))

    def vec_send(tile, count, step):
        send_to = -step * row_tiles + tile + BAND
        return send(vec.at[:, :, pl.ds(tile, count)], win.at[:, :, pl.ds(send_to, count)], at_row(step))

    def vec_pass(source, tile, count, step):
        here = source * row_tiles + tile + BAND
        there = (source - step) * row_tiles + tile + BAND
        return send(win.at[:, :, pl.ds(here, count)], win.at[:, :, pl.ds(there, count)], at_row(step))

    about = []
    for other in others:
        for field, source in enumerate((tile_rows, tile_cols, tile_lats)):
            about.append(send(source, ints.at[ka, field], at_ka(other)))
        about.append(send(own_lives, lives.at[ka], at_ka(other)))

    near_parts = []
    if forwarding:
        second = depth_of(2)
        extra = min(second, row_tiles - 2)
        main = row_tiles - extra
        kept = main - across_tiles
        parts = spans(kept, 2) + [(kept + start, count) for start, count in spans(across_tiles, 2)]

        def part_tile(parity_even, parity_odd, start, count):
            return parity_even * (extra + start) + parity_odd * (main - start - count)

        near_parts.append(vec_send(part_tile(even, odd, *parts[0]), parts[0][1], sign))
        turned = vec_send(odd * (row_tiles - extra), extra, -2 * sign) if extra else None
    hop_parts = []
    hop_spans = spans(slots, max(1, slots // 12))
    for h, other in enumerate(across):
        for start, count in hop_spans:
            hop_parts.append((ka + 2 * (h + 1), start, count, send(
                hop.at[pl.ds(start, count)], all_hop.at[pl.ds(ka * slots + start, count)], at_ka(other))))
    if forwarding:
        for start, count in parts[1:]:
            near_parts.append(vec_send(part_tile(even, odd, start, count), count, sign))
        if extra and not beside_tiles:
            vec_send(odd * (row_tiles - extra), extra, sign)
        vec_send(even * (row_tiles - second), second, 2 * sign)
        if second > extra:
            vec_send(even * extra + odd * (row_tiles - second), second - extra, -2 * sign)
    else:
        first = depth_of(1)
        vec_send(0, first, -1)
        vec_send(row_tiles - first, first, 1)
        if reach >= 2:
            vec_send(0, depth_of(2), -2)
            vec_send(row_tiles - depth_of(2), depth_of(2), 2)
    for d in range(3, reach + 1):
        vec_send(0, depth_of(d), -d)
        vec_send(row_tiles - depth_of(d), depth_of(d), d)
    for start, count in hop_spans:
        send(hop.at[pl.ds(start, count)], all_hop.at[pl.ds(ka * slots + start, count)], at_ka(partner))

    def pass_hop(n):
        owner, start, count, copy = hop_parts[n]
        owner = lax.rem(owner, group_size)
        arrived(copy)
        block = all_hop.at[pl.ds(owner * slots + start, count)]
        send(block, block, at_ka(partner))

    if beside_tiles:
        local[2].wait()
        hold = pltpu.make_async_copy(
            win.at[:, :, pl.ds(BAND + odd * (row_tiles - beside_tiles), beside_tiles)], beside_out, local_sem.at[3])
        hold.start()
        local[2] = hold

    for copy in about:
        arrived(copy)
    for copy in [local[1]] + local[3:]:
        copy.wait()
    del local[3:], local[1]
    make_plan(row_shards, row_tiles, bits, ints, lives, plan)

    done = 0
    if forwarding:
        for n, copy in enumerate(near_parts):
            arrived(copy)
            start, count = parts[n]
            tile = part_tile(odd, even, start, count)
            if start < kept:
                vec_pass(sign, tile, count, 2 * sign)
            else:
                first = part_tile(odd, even, kept, across_tiles)
                hold = pltpu.make_async_copy(
                    win.at[:, :, pl.ds(sign * row_tiles + tile + BAND, count)],
                    across_out.at[:, :, pl.ds(tile - first, count)], local_sem.at[7 + n])
                hold.start()
                local.append(hold)
            if n == 1 and extra:
                arrived(turned)
                vec_pass(2 * sign, odd * (row_tiles - extra), extra, sign)
            until = len(hop_parts) * (n + 1) // (len(near_parts) + 1)
            while done < until:
                pass_hop(done)
                done += 1
        if len(near_parts) < 2 and extra:
            arrived(turned)
            vec_pass(2 * sign, odd * (row_tiles - extra), extra, sign)
    while done < len(hop_parts):
        pass_hop(done)
        done += 1

    for copy in local:
        copy.wait()
    for copy in made:
        if id(copy) not in received:
            copy.wait_recv()
    for copy in made:
        copy.wait_send()


SMEM = pl.BlockSpec(memory_space=pltpu.SMEM)
VMEM = pl.BlockSpec(memory_space=pltpu.VMEM)
ANY = pl.BlockSpec(memory_space=pl.ANY)


def exchange(group_size, row_shards, bits, hop, ints, vec):
    slots = hop.shape[0]
    per_device = ints[0].shape[1]
    row_tiles = vec.shape[2]
    blocks = (group_size * per_device + row_tiles * (GROUP + LATE_GROUP)) // 128 + 1
    width = vec.shape[2] + 2 * BAND
    late = tuple(
        jax.ShapeDtypeStruct(vec.shape[:2] + (count,) + vec.shape[3:], vec.dtype)
        for count in late_tiles(vec.shape[2], row_shards) if count)
    return pl.pallas_call(
        functools.partial(exchange_kernel, group_size, row_shards, bits),
        out_shape=(
            pltpu.VMEM((group_size * slots,) + hop.shape[1:], hop.dtype),
            pltpu.VMEM((blocks + 1, 128), jnp.int32),
            pltpu.VMEM(vec.shape[:2] + (width,) + vec.shape[3:], vec.dtype),
        ) + late,
        in_specs=[ANY] * 4 + [SMEM, ANY],
        out_specs=(pl.BlockSpec(memory_space=pltpu.VMEM), pl.BlockSpec(memory_space=pltpu.VMEM),
                   pl.BlockSpec(memory_space=pltpu.VMEM)) + (pl.BlockSpec(memory_space=pl.ANY),) * len(late),
        scratch_shapes=[
            pltpu.VMEM((group_size, 3, 1, per_device), jnp.int32),
            pltpu.VMEM((group_size, 1, per_device), jnp.int32),
            pltpu.VMEM((1, per_device), jnp.int32),
            pltpu.SemaphoreType.DMA((104,)),
            pltpu.SemaphoreType.DMA((104,)),
            pltpu.SemaphoreType.DMA((16,)),
        ],
        compiler_params=pltpu.CompilerParams(
            collective_id=0, has_side_effects=True, vmem_limit_bytes=4 * 2**20),
        name="exchange",
    )(in_hbm(hop), *map(in_hbm, ints[:3]), ints[3], in_hbm(vec))


def bits_of(count):
    return max(1, (count - 1).bit_length())


def matrix_of(weights, tile, lattice, k):
    cosine = (weights[2 * k, lattice] * tile).astype(jnp.bfloat16)
    sine = (weights[2 * k + 1, lattice] * tile).astype(jnp.bfloat16)
    return jnp.concatenate(
        [jnp.concatenate([cosine, -sine], axis=1), jnp.concatenate([sine, cosine], axis=1)], axis=0)


def unpacked(bits, code):
    tile_bits, place_bits = bits
    return (code & (2**tile_bits - 1), (code >> tile_bits) & (2**place_bits - 1),
            code >> (tile_bits + place_bits))


def push(bits, code, windows, kpoints, register):
    _, place, _ = unpacked(bits, code)
    for k in range(kpoints):
        if len(windows) == 1:
            parts = [windows[0][k, part, place] for part in range(2)]
        else:
            split = windows[0].shape[2]
            near, far = jnp.minimum(place, split - 1), jnp.maximum(place - split, 0)
            parts = [jnp.where(place < split, windows[0][k, part, near], windows[1][k, part, far])
                     for part in range(2)]
        pltpu.matmul_push_rhs(jnp.concatenate(parts, axis=0), staging_register=register, mxu_index=k % 2)


def group(bits, size, at, plan, weights, tiles, windows, accs):
    codes = [plan[lax.div(at + j, 128), lax.rem(at + j, 128)] for j in range(size + 1)]
    for j in range(size):
        push(bits, codes[j + 1], windows, len(accs), (j + 1) % 2)
        index, _, lattice = unpacked(bits, codes[j])
        tile = tiles[index].astype(jnp.float32)
        for k, acc in enumerate(accs):
            pltpu.matmul_acc_lhs(acc, matrix_of(weights, tile, lattice, k), load_staged_rhs=j % 2)


def every_row(bits, size, row_tiles, first, plan, weights, tiles, windows, accs, spare, finish, done=None):
    kpoints = windows[0].shape[0]
    sets = (accs[:kpoints], accs[kpoints:])
    starts = plan.shape[0] - 1

    def one(row, now, before):
        base = plan[starts, first + row]
        groups = lax.div(plan[starts, first + row + 1] - base, size)
        group(bits, size, base, plan, weights, tiles, windows, now)
        finish(jnp.maximum(row - 1, 0), [pltpu.matmul_pop(acc) for acc in before])
        if done is not None:
            @pl.when(row > 0)
            def _():
                done(row - 1)

        def step(g, _):
            group(bits, size, base + g * size, plan, weights, tiles, windows, now)
            return 0

        lax.fori_loop(1, groups, step, 0)

    def pair(i, _):
        one(2 * i, sets[0], sets[1])
        one(2 * i + 1, sets[1], sets[0])
        return 0

    at = plan[starts, first]
    push(bits, plan[lax.div(at, 128), lax.rem(at, 128)], windows, kpoints, 0)
    lax.fori_loop(0, row_tiles // 2, pair, 0)
    if row_tiles % 2:
        one(row_tiles - 1, sets[0], sets[1])
    finish(row_tiles - 1, [pltpu.matmul_pop(acc) for acc in sets[1 - row_tiles % 2]])
    if done is not None:
        done(row_tiles - 1)
    nothing = jnp.zeros((spare[0].shape[0], 256), jnp.bfloat16)
    for acc in spare:
        pltpu.matmul_acc_lhs(acc, nothing, load_staged_rhs=0)
        pltpu.matmul_pop(acc)


def accumulators(kpoints, edge, vec_count):
    return ([pltpu.ACC(k % 2)((2 * edge, vec_count), jnp.float32) for k in range(kpoints)] * 2
            + [pltpu.ACC(k % 2)((16, vec_count), jnp.float32) for k in range(kpoints)])


def first_kernel(bits, plan, weights, tiles, window, total):
    kpoints, _, row_tiles, edge, vec_count = total.shape

    def run(*accs):
        def finish(row, results):
            for k, result in enumerate(results):
                for part in range(2):
                    total[k, part, row] = result[part * edge:(part + 1) * edge]

        every_row(bits, GROUP, row_tiles, 0, plan, weights, tiles, [window], accs[:-kpoints], accs[-kpoints:], finish)

    pl.run_scoped(run, *accumulators(kpoints, edge, vec_count))


def second_kernel(bits, plan, weights, tiles, total, across, beside, out, stage, out_sem):
    kpoints, _, row_tiles, edge, vec_count = total.shape

    def store(row):
        return pltpu.make_async_copy(stage.at[:, :, row], out.at[:, :, row], out_sem.at[row])

    def run(*accs):
        def finish(row, results):
            for k, result in enumerate(results):
                for part in range(2):
                    stage[k, part, row] = total[k, part, row] + result[part * edge:(part + 1) * edge]

        every_row(bits, LATE_GROUP, row_tiles, row_tiles, plan, weights, tiles, [across, beside],
                  accs[:-kpoints], accs[-kpoints:], finish, lambda row: store(row).start())

    pl.run_scoped(run, *accumulators(kpoints, edge, vec_count))
    for row in range(row_tiles):
        store(row).wait()


def in_hbm(x):
    return pltpu.with_memory_space_constraint(x, pltpu.HBM)


def in_vmem(x):
    return pltpu.with_memory_space_constraint(x, pltpu.VMEM)


def first_product(bits, row_tiles, plan, weights, hop, win):
    kpoints, _, _, edge, vec_count = win.shape
    work = hop.shape[0] * kpoints * 8 * edge * edge * vec_count
    return pl.pallas_call(
        functools.partial(first_kernel, bits),
        out_shape=pltpu.VMEM((kpoints, 2, row_tiles, edge, vec_count), jnp.float32),
        in_specs=[SMEM] * 2 + [VMEM] * 2,
        out_specs=VMEM,
        compiler_params=pltpu.CompilerParams(vmem_limit_bytes=2**20),
        cost_estimate=pl.CostEstimate(flops=work, bytes_accessed=2**24, transcendentals=0),
        name="first",
    )(plan, weights, in_vmem(hop), in_vmem(win))


def second_product(bits, plan, weights, hop, total, across, beside):
    row_tiles = total.shape[2]
    return pl.pallas_call(
        functools.partial(second_kernel, bits),
        out_shape=jax.ShapeDtypeStruct(total.shape, jnp.float32),
        in_specs=[SMEM] * 2 + [VMEM] * 4,
        out_specs=ANY,
        scratch_shapes=[
            pltpu.VMEM(total.shape, jnp.float32),
            pltpu.SemaphoreType.DMA((row_tiles,)),
        ],
        compiler_params=pltpu.CompilerParams(vmem_limit_bytes=12 * 2**20),
        name="second",
    )(plan, weights, in_vmem(hop), in_vmem(total), in_vmem(across), in_vmem(beside))


def body(hoppings, tile_rows, tile_cols, tile_lats, tile_counts, phase_angle, vectors):
    edge = hoppings.shape[2]
    group_size = lax.axis_size("ka")
    row_shards = lax.axis_size("rows")
    kpoints, _, orbitals, vec_count = vectors.shape
    lattices = phase_angle.shape[1]
    row_tiles = orbitals // edge
    bits = (bits_of(group_size * hoppings.shape[1]), bits_of(row_tiles + 2 * BAND))
    vec = vectors.reshape(kpoints, 2, row_tiles, edge, vec_count)
    weights = jnp.stack([jnp.cos(phase_angle), jnp.sin(phase_angle)], axis=1).reshape(2 * kpoints, lattices)
    weights = jnp.pad(weights, ((0, 0), (1, 0)))

    ints = (tile_rows, tile_cols, tile_lats, tile_counts)
    all_hop, plan, win, *late = exchange(group_size, row_shards, bits, hoppings[0], ints, vec)
    if late:
        sign = [1 - 2 * (r % 2) for r in range(row_shards)]
        across = lax.ppermute(late[0], "rows", [(r, (r + 2 * sign[r]) % row_shards) for r in range(row_shards)])
        beside = lax.ppermute(late[1], "rows", [(r, r + sign[r]) for r in range(row_shards)])
    total = first_product(bits, row_tiles, plan, weights, all_hop, win)
    if late:
        total = second_product(bits, plan, weights, all_hop, total, across, beside)
    return total.reshape(kpoints, 2, orbitals, vec_count)


def solution(mesh):
    return jax.shard_map(
        body,
        mesh=mesh,
        in_specs=(
            P("rows", "ka", None, None),
            P("rows", "ka"),
            P("rows", "ka"),
            P("rows", "ka"),
            P("rows", "ka"),
            P("ka", None),
            P("ka", None, "rows", None),
        ),
        out_specs=P("ka", None, "rows", None),
        check_vma=False,
    )
```

```python
import functools

import jax
import jax.numpy as jnp
from jax import lax
from jax.experimental import pallas as pl
from jax.experimental.pallas import tpu as pltpu
from jax.sharding import PartitionSpec as P

NLAT = 9
BAND = 16
GROUP = 4
LATE_GROUP = 2
MESH = pl.DeviceIdType.MESH


def spans(total, size):
    return [(start, min(size, total - start)) for start in range(0, total, size)]


def late_stages(row_tiles, row_shards):
    reach = (BAND + row_tiles - 1) // row_tiles
    if row_tiles > BAND or row_shards % 2 or reach < 2:
        return []
    extra = min(row_tiles, BAND - row_tiles, row_tiles - 2)
    late = min(extra, row_tiles - extra)
    first = late - late // 2
    stages = [(row_tiles - extra - late, first, 0, extra - extra // 2)]
    if late // 2 and extra // 2:
        stages.append((row_tiles - extra - late // 2, late // 2, extra - extra // 2, extra // 2))
    else:
        stages = [(row_tiles - extra - late, late, 0, extra)]
    return stages


def column(row):
    size = row.shape[1]
    same = (lax.broadcasted_iota(jnp.int32, (size, size), 0) == lax.broadcasted_iota(jnp.int32, (size, size), 1))
    return jnp.sum(jnp.where(same, jnp.broadcast_to(row, (size, size)), 0.0), axis=1, keepdims=True)


def make_plan(row_shards, row_tiles, bits, ints, lives, plan):
    group_size, _, _, per_device = ints.shape
    stages = late_stages(row_tiles, row_shards)
    dead = (len(stages) + 1) * row_tiles
    shard = lax.axis_index("rows")
    row_start = shard * row_tiles
    total_tiles = row_tiles * row_shards
    odd = lax.rem(shard, 2)
    even = 1 - odd
    low, high = BAND - row_tiles, BAND + 2 * row_tiles
    extra = sum(stage[3] for stage in stages)
    main = row_tiles - extra
    ranges = []
    for number, (across_at, across_tiles, beside_at, beside_tiles) in enumerate(stages):
        ranges.append((number + 1, 0, across_tiles,
                       even * (low + main - across_at - across_tiles) + odd * (high - main + across_at)))
        ranges.append((number + 1, across_tiles, beside_tiles,
                       even * (high - extra + beside_at) + odd * (low + extra - beside_at - beside_tiles)))
    lane = lax.broadcasted_iota(jnp.int32, (1, per_device), 1)

    rows, keys, row_cols, key_cols, code_cols = [], [], [], [], []
    for owner in range(group_size):
        place = ints[owner, 1] - row_start + BAND
        place = jnp.where(place < 0, place + total_tiles, place)
        place = jnp.where(place >= total_tiles, place - total_tiles, place)
        row = ints[owner, 0] - row_start
        inside = place
        for number, shift, count, begin in ranges:
            late = (inside >= begin) & (inside < begin + count)
            row = jnp.where(late, row + number * row_tiles, row)
            place = jnp.where(late, inside - begin + shift, place)
        row = jnp.where(lane < lives[owner], row, dead)
        code = (((ints[owner, 2] + 1) << bits[1]) + place << bits[0]) + owner * per_device + lane
        rows.append(row.astype(jnp.float32))
        keys.append(((row << bits[1]) + place).astype(jnp.float32))
        row_cols.append(column(rows[-1]))
        key_cols.append(column(keys[-1]))
        code_cols.append(column(code.astype(jnp.float32)))
    row_col = jnp.concatenate(row_cols, axis=0)
    key_col = jnp.concatenate(key_cols, axis=0)
    code_col = jnp.concatenate(code_cols, axis=0)
    slots = group_size * per_device
    buckets = -(-(dead + 1) // 8) * 8
    bucket = lax.broadcasted_iota(jnp.int32, (buckets, 1), 0).astype(jnp.float32)
    index = lax.broadcasted_iota(jnp.int32, (slots, 1), 0)
    orders, leads = [], []
    for owner, key in enumerate(keys):
        ahead = (key_col == key) & (index < lane + owner * per_device)
        order = jnp.sum(jnp.where(ahead, 1.0, 0.0), axis=0, keepdims=True)
        live = rows[owner] < dead
        orders.append(order)
        leads.append(jnp.where(live & (order - 2 * jnp.floor(order * 0.5) == 0), 1.0, 0.0))
    order_col = jnp.concatenate([column(order) for order in orders], axis=0)
    lead_col = jnp.concatenate([column(lead) for lead in leads], axis=0)

    held = jnp.zeros((buckets, 1), jnp.float32)
    for row, lead in zip(rows, leads):
        held += jnp.sum(jnp.where(bucket == row, lead, 0.0), axis=1, keepdims=True)
    held = jnp.maximum(held, 1.0)
    held = jnp.where(bucket < row_tiles, jnp.floor((held + (GROUP - 1)) * (1 / GROUP)) * GROUP,
                     jnp.floor((held + (LATE_GROUP - 1)) * (1 / LATE_GROUP)) * LATE_GROUP)
    spots = []
    for owner, (row, lead) in enumerate(zip(rows, leads)):
        ahead = (row_col == row) & (index < lane + owner * per_device)
        rank = jnp.sum(jnp.where(ahead, lead_col, 0.0), axis=0, keepdims=True)
        base = jnp.sum(jnp.where(bucket < row, held, 0.0), axis=0, keepdims=True)
        spots.append(column(jnp.where(lead > 0, base + rank, -1.0)))
    spot = jnp.concatenate(spots, axis=0)
    seconds = []
    for row, key, order, lead in zip(rows, keys, orders, leads):
        led = (key_col == key) & (order_col == order - 1)
        found = jnp.sum(jnp.where(led, spot, 0.0), axis=0, keepdims=True)
        seconds.append(column(jnp.where((lead == 0) & (row < dead), found, -1.0)))
    second = jnp.concatenate(seconds, axis=0)
    wide = lax.broadcasted_iota(jnp.int32, (1, 128), 1)
    blocks = (plan.shape[0] - 1) // 2
    for block in range(blocks):
        here = (wide + block * 128).astype(jnp.float32)
        for line, place in ((block, spot), (blocks + block, second)):
            picked = jnp.sum(jnp.where(place == here, code_col, 0.0), axis=0, keepdims=True)
            plan[line:line + 1] = picked.astype(jnp.int32)
    starts = jnp.sum(jnp.where(bucket < wide.astype(jnp.float32), held, 0.0), axis=0, keepdims=True)
    plan[plan.shape[0] - 1:] = starts.astype(jnp.int32)


def exchange_kernel(group_size, row_shards, bits, hop, tile_rows, tile_cols, tile_lats, tile_counts, vec,
                    all_hop, plan, win, *rest):
    stages = late_stages(vec.shape[2], row_shards)
    across_tiles = sum(stage[1] for stage in stages)
    beside_tiles = sum(stage[3] for stage in stages)
    outs, (ints, lives, own_lives, send_sem, recv_sem, local_sem) = rest[:2 * len(stages)], rest[2 * len(stages):]

    slots = hop.shape[0]
    row_tiles = vec.shape[2]
    own_lives[...] = jnp.full(own_lives.shape, tile_counts[0, 0], jnp.int32)
    ka = lax.axis_index("ka")
    row = lax.axis_index("rows")
    odd = lax.rem(row, 2)
    even = 1 - odd
    sign = 1 - 2 * odd
    partner = ka + 1 - 2 * lax.rem(ka, 2)
    reach = (BAND + row_tiles - 1) // row_tiles
    depth_of = lambda d: min(row_tiles, BAND - (d - 1) * row_tiles)

    def at_row(step):
        return {"ka": ka, "rows": lax.rem(row + step + 2 * row_shards, row_shards)}

    def at_ka(other):
        return {"ka": other, "rows": row}

    across = [lax.rem(ka + 2 * h, group_size) for h in range(1, group_size // 2)]
    others = [lax.rem(ka + h, group_size) for h in range(1, group_size)]
    forwarding = row_tiles <= BAND and row_shards % 2 == 0 and reach >= 2
    peers = [at_ka(o) for o in others]
    if forwarding:
        peers.append(at_row(sign))
    else:
        peers += [at_row(1), at_row(-1)]
    for d in range(2, reach + 1):
        peers += [at_row(d), at_row(-d)]

    barrier = pltpu.get_barrier_semaphore()
    for peer in peers:
        pl.semaphore_signal(barrier, inc=1, device_id=peer, device_id_type=MESH)

    local = [
        pltpu.make_async_copy(hop, all_hop.at[pl.ds(ka * slots, slots)], local_sem.at[0]),
        pltpu.make_async_copy(own_lives, lives.at[ka], local_sem.at[1]),
        pltpu.make_async_copy(vec, win.at[:, :, pl.ds(BAND, row_tiles)], local_sem.at[2]),
    ]
    for field, source in enumerate((tile_rows, tile_cols, tile_lats)):
        local.append(pltpu.make_async_copy(source, ints.at[ka, field], local_sem.at[4 + field]))
    for copy in [local[0]] + local[2:]:
        copy.start()
    pl.semaphore_wait(barrier, len(peers))
    local[1].start()

    made = []

    def send(src, dst, device):
        n = len(made)
        copy = pltpu.make_async_remote_copy(
            src_ref=src, dst_ref=dst, send_sem=send_sem.at[n], recv_sem=recv_sem.at[n],
            device_id=device, device_id_type=MESH)
        copy.start()
        made.append(copy)
        return copy

    received = set()

    def arrived(copy):
        copy.wait_recv()
        received.add(id(copy))

    def vec_send(tile, count, step):
        send_to = -step * row_tiles + tile + BAND
        return send(vec.at[:, :, pl.ds(tile, count)], win.at[:, :, pl.ds(send_to, count)], at_row(step))

    def vec_pass(source, tile, count, step):
        here = source * row_tiles + tile + BAND
        there = (source - step) * row_tiles + tile + BAND
        return send(win.at[:, :, pl.ds(here, count)], win.at[:, :, pl.ds(there, count)], at_row(step))

    about = []
    for other in others:
        for field, source in enumerate((tile_rows, tile_cols, tile_lats)):
            about.append(send(source, ints.at[ka, field], at_ka(other)))
        about.append(send(own_lives, lives.at[ka], at_ka(other)))

    near_parts = []
    if forwarding:
        second = depth_of(2)
        extra = min(second, row_tiles - 2)
        main = row_tiles - extra
        kept = main - across_tiles
        parts = [(start, count, None) for start, count in spans(kept, 2)]
        for number, (at, tiles, _, _) in enumerate(stages):
            parts += [(at + start, count, number) for start, count in spans(tiles, 2)]

        def part_tile(parity_even, parity_odd, start, count):
            return parity_even * (extra + start) + parity_odd * (main - start - count)

        near_parts.append(vec_send(part_tile(even, odd, *parts[0][:2]), parts[0][1], sign))
        turned = vec_send(odd * (row_tiles - extra), extra, -2 * sign) if extra else None
    hop_parts = []
    hop_spans = spans(slots, max(1, slots // 12))
    for h, other in enumerate(across):
        for start, count in hop_spans:
            hop_parts.append((ka + 2 * (h + 1), start, count, send(
                hop.at[pl.ds(start, count)], all_hop.at[pl.ds(ka * slots + start, count)], at_ka(other))))
    if forwarding:
        for start, count, _ in parts[1:]:
            near_parts.append(vec_send(part_tile(even, odd, start, count), count, sign))
        if extra and not beside_tiles:
            vec_send(odd * (row_tiles - extra), extra, sign)
        vec_send(even * (row_tiles - second), second, 2 * sign)
        if second > extra:
            vec_send(even * extra + odd * (row_tiles - second), second - extra, -2 * sign)
    else:
        first = depth_of(1)
        vec_send(0, first, -1)
        vec_send(row_tiles - first, first, 1)
        if reach >= 2:
            vec_send(0, depth_of(2), -2)
            vec_send(row_tiles - depth_of(2), depth_of(2), 2)
    for d in range(3, reach + 1):
        vec_send(0, depth_of(d), -d)
        vec_send(row_tiles - depth_of(d), depth_of(d), d)
    for start, count in hop_spans:
        send(hop.at[pl.ds(start, count)], all_hop.at[pl.ds(ka * slots + start, count)], at_ka(partner))

    def pass_hop(n):
        owner, start, count, copy = hop_parts[n]
        owner = lax.rem(owner, group_size)
        arrived(copy)
        block = all_hop.at[pl.ds(owner * slots + start, count)]
        send(block, block, at_ka(partner))

    holds = []
    if stages:
        local[2].wait()
        for number, (_, _, at, count) in enumerate(stages):
            tile = even * (beside_tiles - at - count) + odd * (row_tiles - beside_tiles + at)
            holds.append(pltpu.make_async_copy(
                win.at[:, :, pl.ds(BAND + tile, count)], outs[2 * number + 1], local_sem.at[7 + number]))
            holds[-1].start()

    for copy in about:
        arrived(copy)
    for copy in [local[1]] + local[3:]:
        copy.wait()
    local = [local[0]] + (holds or [local[2]])
    make_plan(row_shards, row_tiles, bits, ints, lives, plan)

    done = 0
    if forwarding:
        for n, copy in enumerate(near_parts):
            arrived(copy)
            start, count, number = parts[n]
            tile = part_tile(odd, even, start, count)
            if number is None:
                vec_pass(sign, tile, count, 2 * sign)
            else:
                first = part_tile(odd, even, *stages[number][:2])
                hold = pltpu.make_async_copy(
                    win.at[:, :, pl.ds(sign * row_tiles + tile + BAND, count)],
                    outs[2 * number].at[:, :, pl.ds(tile - first, count)], local_sem.at[10 + n])
                hold.start()
                local.append(hold)
            if n == 1 and extra:
                arrived(turned)
                vec_pass(2 * sign, odd * (row_tiles - extra), extra, sign)
            until = len(hop_parts) * (n + 1) // (len(near_parts) + 1)
            while done < until:
                pass_hop(done)
                done += 1
        if len(near_parts) < 2 and extra:
            arrived(turned)
            vec_pass(2 * sign, odd * (row_tiles - extra), extra, sign)
    while done < len(hop_parts):
        pass_hop(done)
        done += 1

    for copy in local:
        copy.wait()
    for copy in made:
        if id(copy) not in received:
            copy.wait_recv()
    for copy in made:
        copy.wait_send()


SMEM = pl.BlockSpec(memory_space=pltpu.SMEM)
VMEM = pl.BlockSpec(memory_space=pltpu.VMEM)
ANY = pl.BlockSpec(memory_space=pl.ANY)


def exchange(group_size, row_shards, bits, hop, ints, vec):
    slots = hop.shape[0]
    per_device = ints[0].shape[1]
    row_tiles = vec.shape[2]
    blocks = (group_size * per_device + row_tiles * (GROUP + 2 * LATE_GROUP)) // 128 + 1
    width = vec.shape[2] + 2 * BAND
    stages = late_stages(row_tiles, row_shards)
    late = tuple(
        jax.ShapeDtypeStruct(vec.shape[:2] + (count,) + vec.shape[3:], vec.dtype)
        for _, across, _, beside in stages for count in (across, beside))
    return pl.pallas_call(
        functools.partial(exchange_kernel, group_size, row_shards, bits),
        out_shape=(
            pltpu.VMEM((group_size * slots,) + hop.shape[1:], hop.dtype),
            pltpu.VMEM((2 * blocks + 1, 128), jnp.int32),
            pltpu.VMEM(vec.shape[:2] + (width,) + vec.shape[3:], vec.dtype),
        ) + late,
        in_specs=[ANY] * 4 + [SMEM, ANY],
        out_specs=(pl.BlockSpec(memory_space=pltpu.VMEM), pl.BlockSpec(memory_space=pltpu.VMEM),
                   pl.BlockSpec(memory_space=pltpu.VMEM)) + (pl.BlockSpec(memory_space=pl.ANY),) * len(late),
        scratch_shapes=[
            pltpu.VMEM((group_size, 3, 1, per_device), jnp.int32),
            pltpu.VMEM((group_size, 1, per_device), jnp.int32),
            pltpu.VMEM((1, per_device), jnp.int32),
            pltpu.SemaphoreType.DMA((104,)),
            pltpu.SemaphoreType.DMA((104,)),
            pltpu.SemaphoreType.DMA((24,)),
        ],
        compiler_params=pltpu.CompilerParams(
            collective_id=0, has_side_effects=True, vmem_limit_bytes=4 * 2**20),
        name="exchange",
    )(in_hbm(hop), *map(in_hbm, ints[:3]), ints[3], in_hbm(vec))


def bits_of(count):
    return max(1, (count - 1).bit_length())


def matrix_of(cosine, sine):
    cosine, sine = cosine.astype(jnp.bfloat16), sine.astype(jnp.bfloat16)
    return jnp.concatenate(
        [jnp.concatenate([cosine, -sine], axis=1), jnp.concatenate([sine, cosine], axis=1)], axis=0)


def unpacked(bits, code):
    tile_bits, place_bits = bits
    return (code & (2**tile_bits - 1), (code >> tile_bits) & (2**place_bits - 1),
            code >> (tile_bits + place_bits))


def push(bits, code, windows, kpoints, register):
    _, place, _ = unpacked(bits, code)
    for k in range(kpoints):
        if len(windows) == 1:
            parts = [windows[0][k, part, place] for part in range(2)]
        else:
            split = windows[0].shape[2]
            near, far = jnp.minimum(place, split - 1), jnp.maximum(place - split, 0)
            parts = [jnp.where(place < split, windows[0][k, part, near], windows[1][k, part, far])
                     for part in range(2)]
        pltpu.matmul_push_rhs(jnp.concatenate(parts, axis=0), staging_register=register, mxu_index=k % 2)


def group(bits, size, at, plan, weights, tiles, windows, accs):
    blocks = (plan.shape[0] - 1) // 2
    lines = [(lax.div(at + j, 128), lax.rem(at + j, 128)) for j in range(size + 1)]
    codes = [plan[line, lane] for line, lane in lines]
    for j in range(size):
        push(bits, codes[j + 1], windows, len(accs), (j + 1) % 2)
        index, _, lattice = unpacked(bits, codes[j])
        other, _, other_lattice = unpacked(bits, plan[blocks + lines[j][0], lines[j][1]])
        tile = tiles[index].astype(jnp.float32)
        beside = tiles[other].astype(jnp.float32)
        for k, acc in enumerate(accs):
            cosine, sine = [weights[2 * k + part, lattice] * tile + weights[2 * k + part, other_lattice] * beside
                            for part in range(2)]
            pltpu.matmul_acc_lhs(acc, matrix_of(cosine, sine), load_staged_rhs=j % 2)


def every_row(bits, size, row_tiles, first, plan, weights, tiles, windows, accs, spare, finish, done=None):
    kpoints = windows[0].shape[0]
    sets = (accs[:kpoints], accs[kpoints:])
    starts = plan.shape[0] - 1

    def one(row, now, before):
        base = plan[starts, first + row]
        groups = lax.div(plan[starts, first + row + 1] - base, size)
        group(bits, size, base, plan, weights, tiles, windows, now)
        finish(jnp.maximum(row - 1, 0), [pltpu.matmul_pop(acc) for acc in before])
        if done is not None:
            @pl.when(row > 0)
            def _():
                done(row - 1)

        def step(g, _):
            group(bits, size, base + g * size, plan, weights, tiles, windows, now)
            return 0

        lax.fori_loop(1, groups, step, 0)

    def pair(i, _):
        one(2 * i, sets[0], sets[1])
        one(2 * i + 1, sets[1], sets[0])
        return 0

    at = plan[starts, first]
    push(bits, plan[lax.div(at, 128), lax.rem(at, 128)], windows, kpoints, 0)
    lax.fori_loop(0, row_tiles // 2, pair, 0)
    if row_tiles % 2:
        one(row_tiles - 1, sets[0], sets[1])
    finish(row_tiles - 1, [pltpu.matmul_pop(acc) for acc in sets[1 - row_tiles % 2]])
    if done is not None:
        done(row_tiles - 1)
    nothing = jnp.zeros((spare[0].shape[0], 256), jnp.bfloat16)
    for acc in spare:
        pltpu.matmul_acc_lhs(acc, nothing, load_staged_rhs=0)
        pltpu.matmul_pop(acc)


def accumulators(kpoints, edge, vec_count):
    return ([pltpu.ACC(k % 2)((2 * edge, vec_count), jnp.float32) for k in range(kpoints)] * 2
            + [pltpu.ACC(k % 2)((16, vec_count), jnp.float32) for k in range(kpoints)])


def first_kernel(bits, plan, weights, tiles, window, total):
    kpoints, _, row_tiles, edge, vec_count = total.shape

    def run(*accs):
        def finish(row, results):
            for k, result in enumerate(results):
                for part in range(2):
                    total[k, part, row] = result[part * edge:(part + 1) * edge]

        every_row(bits, GROUP, row_tiles, 0, plan, weights, tiles, [window], accs[:-kpoints], accs[-kpoints:], finish)

    pl.run_scoped(run, *accumulators(kpoints, edge, vec_count))


def late_kernel(bits, stage_number, last, plan, weights, tiles, total, across, beside, out, *scratch):
    kpoints, _, row_tiles, edge, vec_count = total.shape
    stage, out_sem = scratch if last else (out, None)

    def store(row):
        return pltpu.make_async_copy(stage.at[:, :, row], out.at[:, :, row], out_sem.at[row])

    def run(*accs):
        def finish(row, results):
            for k, result in enumerate(results):
                for part in range(2):
                    stage[k, part, row] = total[k, part, row] + result[part * edge:(part + 1) * edge]

        every_row(bits, LATE_GROUP, row_tiles, stage_number * row_tiles, plan, weights, tiles, [across, beside],
                  accs[:-kpoints], accs[-kpoints:], finish, (lambda row: store(row).start()) if last else None)

    pl.run_scoped(run, *accumulators(kpoints, edge, vec_count))
    if last:
        for row in range(row_tiles):
            store(row).wait()


def in_hbm(x):
    return pltpu.with_memory_space_constraint(x, pltpu.HBM)


def in_vmem(x):
    return pltpu.with_memory_space_constraint(x, pltpu.VMEM)


def first_product(bits, row_tiles, plan, weights, hop, win):
    kpoints, _, _, edge, vec_count = win.shape
    work = hop.shape[0] * kpoints * 8 * edge * edge * vec_count
    return pl.pallas_call(
        functools.partial(first_kernel, bits),
        out_shape=pltpu.VMEM((kpoints, 2, row_tiles, edge, vec_count), jnp.float32),
        in_specs=[SMEM] * 2 + [VMEM] * 2,
        out_specs=VMEM,
        compiler_params=pltpu.CompilerParams(vmem_limit_bytes=2**20),
        cost_estimate=pl.CostEstimate(flops=work, bytes_accessed=2**24, transcendentals=0),
        name="first",
    )(plan, weights, in_vmem(hop), in_vmem(win))


def late_product(bits, number, last, plan, weights, hop, total, across, beside):
    row_tiles = total.shape[2]
    work = hop.shape[0] * total.size // 2
    return pl.pallas_call(
        functools.partial(late_kernel, bits, number, last),
        out_shape=(jax.ShapeDtypeStruct if last else pltpu.VMEM)(total.shape, jnp.float32),
        in_specs=[SMEM] * 2 + [VMEM] * 4,
        out_specs=ANY if last else VMEM,
        scratch_shapes=[
            pltpu.VMEM(total.shape, jnp.float32),
            pltpu.SemaphoreType.DMA((row_tiles,)),
        ] if last else [],
        compiler_params=pltpu.CompilerParams(vmem_limit_bytes=(12 if last else 2) * 2**20),
        cost_estimate=pl.CostEstimate(flops=work, bytes_accessed=2**22, transcendentals=0),
        name="late",
    )(plan, weights, in_vmem(hop), in_vmem(total), in_vmem(across), in_vmem(beside))


def body(hoppings, tile_rows, tile_cols, tile_lats, tile_counts, phase_angle, vectors):
    edge = hoppings.shape[2]
    group_size = lax.axis_size("ka")
    row_shards = lax.axis_size("rows")
    kpoints, _, orbitals, vec_count = vectors.shape
    lattices = phase_angle.shape[1]
    row_tiles = orbitals // edge
    bits = (bits_of(group_size * hoppings.shape[1]), bits_of(row_tiles + 2 * BAND))
    vec = vectors.reshape(kpoints, 2, row_tiles, edge, vec_count)
    weights = jnp.stack([jnp.cos(phase_angle), jnp.sin(phase_angle)], axis=1).reshape(2 * kpoints, lattices)
    weights = jnp.pad(weights, ((0, 0), (1, 0)))

    ints = (tile_rows, tile_cols, tile_lats, tile_counts)
    all_hop, plan, win, *late = exchange(group_size, row_shards, bits, hoppings[0], ints, vec)
    sign = [1 - 2 * (r % 2) for r in range(row_shards)]
    far = [(r, (r + 2 * sign[r]) % row_shards) for r in range(row_shards)]
    pairs = [(r, r + sign[r]) for r in range(row_shards)]
    moved = [lax.ppermute(x, "rows", pairs if n % 2 else far) for n, x in enumerate(late)]
    total = first_product(bits, row_tiles, plan, weights, all_hop, win)
    for n in range(0, len(moved), 2):
        total = late_product(bits, n // 2 + 1, n + 2 == len(moved), plan, weights, all_hop, total, *moved[n:n + 2])
    return total.reshape(kpoints, 2, orbitals, vec_count)


def solution(mesh):
    return jax.shard_map(
        body,
        mesh=mesh,
        in_specs=(
            P("rows", "ka", None, None),
            P("rows", "ka"),
            P("rows", "ka"),
            P("rows", "ka"),
            P("rows", "ka"),
            P("ka", None),
            P("ka", None, "rows", None),
        ),
        out_specs=P("ka", None, "rows", None),
        check_vma=False,
    )
```

```python
import functools

import jax
import jax.numpy as jnp
from jax import lax
from jax.experimental import pallas as pl
from jax.experimental.pallas import tpu as pltpu
from jax.sharding import PartitionSpec as P

NLAT = 9
BAND = 16
GROUP = 4
LATE_GROUP = 1
MESH = pl.DeviceIdType.MESH


def spans(total, size):
    return [(start, min(size, total - start)) for start in range(0, total, size)]


def late_stages(row_tiles, row_shards):
    reach = (BAND + row_tiles - 1) // row_tiles
    if row_tiles > BAND or row_shards % 2 or reach < 2:
        return []
    extra = min(row_tiles, BAND - row_tiles, row_tiles - 2)
    late = min(extra, row_tiles - extra)
    first = late - late // 2
    stages = [(row_tiles - extra - late, first, 0, extra - extra // 2)]
    if late // 2 and extra // 2:
        stages.append((row_tiles - extra - late // 2, late // 2, extra - extra // 2, extra // 2))
    else:
        stages = [(row_tiles - extra - late, late, 0, extra)]
    return stages


def column(row):
    size = row.shape[1]
    same = (lax.broadcasted_iota(jnp.int32, (size, size), 0) == lax.broadcasted_iota(jnp.int32, (size, size), 1))
    return jnp.sum(jnp.where(same, jnp.broadcast_to(row, (size, size)), 0.0), axis=1, keepdims=True)


def make_plan(row_shards, row_tiles, bits, ints, lives, plan):
    group_size, _, _, per_device = ints.shape
    stages = late_stages(row_tiles, row_shards)
    dead = (len(stages) + 1) * row_tiles
    shard = lax.axis_index("rows")
    row_start = shard * row_tiles
    total_tiles = row_tiles * row_shards
    odd = lax.rem(shard, 2)
    even = 1 - odd
    low, high = BAND - row_tiles, BAND + 2 * row_tiles
    extra = sum(stage[3] for stage in stages)
    main = row_tiles - extra
    ranges = []
    for number, (across_at, across_tiles, beside_at, beside_tiles) in enumerate(stages):
        ranges.append((number + 1, 0, across_tiles,
                       even * (low + main - across_at - across_tiles) + odd * (high - main + across_at)))
        ranges.append((number + 1, across_tiles, beside_tiles,
                       even * (high - extra + beside_at) + odd * (low + extra - beside_at - beside_tiles)))
    lane = lax.broadcasted_iota(jnp.int32, (1, per_device), 1)

    rows, keys, row_cols, key_cols, code_cols = [], [], [], [], []
    for owner in range(group_size):
        place = ints[owner, 1] - row_start + BAND
        place = jnp.where(place < 0, place + total_tiles, place)
        place = jnp.where(place >= total_tiles, place - total_tiles, place)
        row = ints[owner, 0] - row_start
        inside = place
        for number, shift, count, begin in ranges:
            late = (inside >= begin) & (inside < begin + count)
            row = jnp.where(late, row + number * row_tiles, row)
            place = jnp.where(late, inside - begin + shift, place)
        row = jnp.where(lane < lives[owner], row, dead)
        code = (((ints[owner, 2] + 1) << bits[1]) + place << bits[0]) + owner * per_device + lane
        rows.append(row.astype(jnp.float32))
        keys.append(((row << bits[1]) + place).astype(jnp.float32))
        row_cols.append(column(rows[-1]))
        key_cols.append(column(keys[-1]))
        code_cols.append(column(code.astype(jnp.float32)))
    row_col = jnp.concatenate(row_cols, axis=0)
    key_col = jnp.concatenate(key_cols, axis=0)
    code_col = jnp.concatenate(code_cols, axis=0)
    slots = group_size * per_device
    buckets = -(-(dead + 1) // 8) * 8
    bucket = lax.broadcasted_iota(jnp.int32, (buckets, 1), 0).astype(jnp.float32)
    index = lax.broadcasted_iota(jnp.int32, (slots, 1), 0)
    orders, leads = [], []
    for owner, key in enumerate(keys):
        ahead = (key_col == key) & (index < lane + owner * per_device)
        order = jnp.sum(jnp.where(ahead, 1.0, 0.0), axis=0, keepdims=True)
        live = rows[owner] < dead
        orders.append(order)
        leads.append(jnp.where(live & (order - 2 * jnp.floor(order * 0.5) == 0), 1.0, 0.0))
    order_col = jnp.concatenate([column(order) for order in orders], axis=0)
    lead_col = jnp.concatenate([column(lead) for lead in leads], axis=0)

    held = jnp.zeros((buckets, 1), jnp.float32)
    for row, lead in zip(rows, leads):
        held += jnp.sum(jnp.where(bucket == row, lead, 0.0), axis=1, keepdims=True)
    held = jnp.maximum(held, 1.0)
    held = jnp.where(bucket < row_tiles, jnp.floor((held + (GROUP - 1)) * (1 / GROUP)) * GROUP,
                     jnp.floor((held + (LATE_GROUP - 1)) * (1 / LATE_GROUP)) * LATE_GROUP)
    spots = []
    for owner, (row, lead) in enumerate(zip(rows, leads)):
        ahead = (row_col == row) & (index < lane + owner * per_device)
        rank = jnp.sum(jnp.where(ahead, lead_col, 0.0), axis=0, keepdims=True)
        base = jnp.sum(jnp.where(bucket < row, held, 0.0), axis=0, keepdims=True)
        spots.append(column(jnp.where(lead > 0, base + rank, -1.0)))
    spot = jnp.concatenate(spots, axis=0)
    seconds = []
    for row, key, order, lead in zip(rows, keys, orders, leads):
        led = (key_col == key) & (order_col == order - 1)
        found = jnp.sum(jnp.where(led, spot, 0.0), axis=0, keepdims=True)
        seconds.append(column(jnp.where((lead == 0) & (row < dead), found, -1.0)))
    second = jnp.concatenate(seconds, axis=0)
    wide = lax.broadcasted_iota(jnp.int32, (1, 128), 1)
    blocks = (plan.shape[0] - 1) // 2
    for block in range(blocks):
        here = (wide + block * 128).astype(jnp.float32)
        for line, place in ((block, spot), (blocks + block, second)):
            picked = jnp.sum(jnp.where(place == here, code_col, 0.0), axis=0, keepdims=True)
            plan[line:line + 1] = picked.astype(jnp.int32)
    starts = jnp.sum(jnp.where(bucket < wide.astype(jnp.float32), held, 0.0), axis=0, keepdims=True)
    plan[plan.shape[0] - 1:] = starts.astype(jnp.int32)


def exchange_kernel(group_size, row_shards, bits, hop, tile_rows, tile_cols, tile_lats, tile_counts, vec,
                    all_hop, plan, win, *rest):
    stages = late_stages(vec.shape[2], row_shards)
    across_tiles = sum(stage[1] for stage in stages)
    beside_tiles = sum(stage[3] for stage in stages)
    outs, (ints, lives, own_lives, send_sem, recv_sem, local_sem) = rest[:2 * len(stages)], rest[2 * len(stages):]

    slots = hop.shape[0]
    row_tiles = vec.shape[2]
    own_lives[...] = jnp.full(own_lives.shape, tile_counts[0, 0], jnp.int32)
    ka = lax.axis_index("ka")
    row = lax.axis_index("rows")
    odd = lax.rem(row, 2)
    even = 1 - odd
    sign = 1 - 2 * odd
    partner = ka + 1 - 2 * lax.rem(ka, 2)
    reach = (BAND + row_tiles - 1) // row_tiles
    depth_of = lambda d: min(row_tiles, BAND - (d - 1) * row_tiles)

    def at_row(step):
        return {"ka": ka, "rows": lax.rem(row + step + 2 * row_shards, row_shards)}

    def at_ka(other):
        return {"ka": other, "rows": row}

    across = [lax.rem(ka + 2 * h, group_size) for h in range(1, group_size // 2)]
    others = [lax.rem(ka + h, group_size) for h in range(1, group_size)]
    forwarding = row_tiles <= BAND and row_shards % 2 == 0 and reach >= 2
    peers = [at_ka(o) for o in others]
    if forwarding:
        peers.append(at_row(sign))
    else:
        peers += [at_row(1), at_row(-1)]
    for d in range(2, reach + 1):
        peers += [at_row(d), at_row(-d)]

    barrier = pltpu.get_barrier_semaphore()
    for peer in peers:
        pl.semaphore_signal(barrier, inc=1, device_id=peer, device_id_type=MESH)

    local = [
        pltpu.make_async_copy(hop, all_hop.at[pl.ds(ka * slots, slots)], local_sem.at[0]),
        pltpu.make_async_copy(own_lives, lives.at[ka], local_sem.at[1]),
        pltpu.make_async_copy(vec, win.at[:, :, pl.ds(BAND, row_tiles)], local_sem.at[2]),
    ]
    for field, source in enumerate((tile_rows, tile_cols, tile_lats)):
        local.append(pltpu.make_async_copy(source, ints.at[ka, field], local_sem.at[4 + field]))
    for copy in [local[0]] + local[2:]:
        copy.start()
    pl.semaphore_wait(barrier, len(peers))
    local[1].start()

    made = []

    def send(src, dst, device):
        n = len(made)
        copy = pltpu.make_async_remote_copy(
            src_ref=src, dst_ref=dst, send_sem=send_sem.at[n], recv_sem=recv_sem.at[n],
            device_id=device, device_id_type=MESH)
        copy.start()
        made.append(copy)
        return copy

    received = set()

    def arrived(copy):
        copy.wait_recv()
        received.add(id(copy))

    def vec_send(tile, count, step):
        send_to = -step * row_tiles + tile + BAND
        return send(vec.at[:, :, pl.ds(tile, count)], win.at[:, :, pl.ds(send_to, count)], at_row(step))

    def vec_pass(source, tile, count, step):
        here = source * row_tiles + tile + BAND
        there = (source - step) * row_tiles + tile + BAND
        return send(win.at[:, :, pl.ds(here, count)], win.at[:, :, pl.ds(there, count)], at_row(step))

    about = []
    for other in others:
        for field, source in enumerate((tile_rows, tile_cols, tile_lats)):
            about.append(send(source, ints.at[ka, field], at_ka(other)))
        about.append(send(own_lives, lives.at[ka], at_ka(other)))

    near_parts = []
    if forwarding:
        second = depth_of(2)
        extra = min(second, row_tiles - 2)
        main = row_tiles - extra
        kept = main - across_tiles
        parts = [(start, count, None) for start, count in spans(kept, 2)]
        for number, (at, tiles, _, _) in enumerate(stages):
            parts += [(at + start, count, number) for start, count in spans(tiles, 2)]

        def part_tile(parity_even, parity_odd, start, count):
            return parity_even * (extra + start) + parity_odd * (main - start - count)

        near_parts.append(vec_send(part_tile(even, odd, *parts[0][:2]), parts[0][1], sign))
        turned = vec_send(odd * (row_tiles - extra), extra, -2 * sign) if extra else None
    hop_parts = []
    hop_spans = spans(slots, max(1, slots // 24))
    for h, other in enumerate(across):
        for start, count in hop_spans:
            hop_parts.append((ka + 2 * (h + 1), start, count, send(
                hop.at[pl.ds(start, count)], all_hop.at[pl.ds(ka * slots + start, count)], at_ka(other))))
    if forwarding:
        for start, count, _ in parts[1:]:
            near_parts.append(vec_send(part_tile(even, odd, start, count), count, sign))
        if extra and not beside_tiles:
            vec_send(odd * (row_tiles - extra), extra, sign)
        vec_send(even * (row_tiles - second), second, 2 * sign)
        if second > extra:
            vec_send(even * extra + odd * (row_tiles - second), second - extra, -2 * sign)
    else:
        first = depth_of(1)
        vec_send(0, first, -1)
        vec_send(row_tiles - first, first, 1)
        if reach >= 2:
            vec_send(0, depth_of(2), -2)
            vec_send(row_tiles - depth_of(2), depth_of(2), 2)
    for d in range(3, reach + 1):
        vec_send(0, depth_of(d), -d)
        vec_send(row_tiles - depth_of(d), depth_of(d), d)
    for start, count in hop_spans:
        send(hop.at[pl.ds(start, count)], all_hop.at[pl.ds(ka * slots + start, count)], at_ka(partner))

    def pass_hop(n):
        owner, start, count, copy = hop_parts[n]
        owner = lax.rem(owner, group_size)
        arrived(copy)
        block = all_hop.at[pl.ds(owner * slots + start, count)]
        send(block, block, at_ka(partner))

    holds = []
    if stages:
        local[2].wait()
        for number, (_, _, at, count) in enumerate(stages):
            tile = even * (beside_tiles - at - count) + odd * (row_tiles - beside_tiles + at)
            holds.append(pltpu.make_async_copy(
                win.at[:, :, pl.ds(BAND + tile, count)], outs[2 * number + 1], local_sem.at[7 + number]))
            holds[-1].start()

    for copy in about:
        arrived(copy)
    for copy in [local[1]] + local[3:]:
        copy.wait()
    local = [local[0]] + (holds or [local[2]])
    make_plan(row_shards, row_tiles, bits, ints, lives, plan)

    done = 0
    if forwarding:
        for n, copy in enumerate(near_parts):
            arrived(copy)
            start, count, number = parts[n]
            tile = part_tile(odd, even, start, count)
            if number is None:
                vec_pass(sign, tile, count, 2 * sign)
            else:
                first = part_tile(odd, even, *stages[number][:2])
                hold = pltpu.make_async_copy(
                    win.at[:, :, pl.ds(sign * row_tiles + tile + BAND, count)],
                    outs[2 * number].at[:, :, pl.ds(tile - first, count)], local_sem.at[10 + n])
                hold.start()
                local.append(hold)
            if n == 1 and extra:
                arrived(turned)
                vec_pass(2 * sign, odd * (row_tiles - extra), extra, sign)
            until = len(hop_parts) * (n + 1) // (len(near_parts) + 1)
            while done < until:
                pass_hop(done)
                done += 1
        if len(near_parts) < 2 and extra:
            arrived(turned)
            vec_pass(2 * sign, odd * (row_tiles - extra), extra, sign)
    while done < len(hop_parts):
        pass_hop(done)
        done += 1

    for copy in local:
        copy.wait()
    for copy in made:
        if id(copy) not in received:
            copy.wait_recv()
    for copy in made:
        copy.wait_send()


SMEM = pl.BlockSpec(memory_space=pltpu.SMEM)
VMEM = pl.BlockSpec(memory_space=pltpu.VMEM)
ANY = pl.BlockSpec(memory_space=pl.ANY)


def exchange(group_size, row_shards, bits, hop, ints, vec):
    slots = hop.shape[0]
    per_device = ints[0].shape[1]
    row_tiles = vec.shape[2]
    blocks = (group_size * per_device + row_tiles * (GROUP + 2 * LATE_GROUP)) // 128 + 1
    width = vec.shape[2] + 2 * BAND
    stages = late_stages(row_tiles, row_shards)
    late = tuple(
        jax.ShapeDtypeStruct(vec.shape[:2] + (count,) + vec.shape[3:], vec.dtype)
        for _, across, _, beside in stages for count in (across, beside))
    return pl.pallas_call(
        functools.partial(exchange_kernel, group_size, row_shards, bits),
        out_shape=(
            pltpu.VMEM((group_size * slots,) + hop.shape[1:], hop.dtype),
            pltpu.VMEM((2 * blocks + 1, 128), jnp.int32),
            pltpu.VMEM(vec.shape[:2] + (width,) + vec.shape[3:], vec.dtype),
        ) + late,
        in_specs=[ANY] * 4 + [SMEM, ANY],
        out_specs=(pl.BlockSpec(memory_space=pltpu.VMEM), pl.BlockSpec(memory_space=pltpu.VMEM),
                   pl.BlockSpec(memory_space=pltpu.VMEM)) + (pl.BlockSpec(memory_space=pl.ANY),) * len(late),
        scratch_shapes=[
            pltpu.VMEM((group_size, 3, 1, per_device), jnp.int32),
            pltpu.VMEM((group_size, 1, per_device), jnp.int32),
            pltpu.VMEM((1, per_device), jnp.int32),
            pltpu.SemaphoreType.DMA((104,)),
            pltpu.SemaphoreType.DMA((104,)),
            pltpu.SemaphoreType.DMA((24,)),
        ],
        compiler_params=pltpu.CompilerParams(
            collective_id=0, has_side_effects=True, vmem_limit_bytes=4 * 2**20),
        name="exchange",
    )(in_hbm(hop), *map(in_hbm, ints[:3]), ints[3], in_hbm(vec))


def bits_of(count):
    return max(1, (count - 1).bit_length())


def matrix_of(cosine, sine):
    cosine, sine = cosine.astype(jnp.bfloat16), sine.astype(jnp.bfloat16)
    return jnp.concatenate(
        [jnp.concatenate([cosine, -sine], axis=1), jnp.concatenate([sine, cosine], axis=1)], axis=0)


def unpacked(bits, code):
    tile_bits, place_bits = bits
    return (code & (2**tile_bits - 1), (code >> tile_bits) & (2**place_bits - 1),
            code >> (tile_bits + place_bits))


def push(bits, code, windows, kpoints, register):
    _, place, _ = unpacked(bits, code)
    for k in range(kpoints):
        if len(windows) == 1:
            parts = [windows[0][k, part, place] for part in range(2)]
        else:
            split = windows[0].shape[2]
            near, far = jnp.minimum(place, split - 1), jnp.maximum(place - split, 0)
            parts = [jnp.where(place < split, windows[0][k, part, near], windows[1][k, part, far])
                     for part in range(2)]
        pltpu.matmul_push_rhs(jnp.concatenate(parts, axis=0), staging_register=register, mxu_index=k % 2)


def group(bits, size, at, plan, weights, tiles, windows, accs):
    blocks = (plan.shape[0] - 1) // 2
    lines = [(lax.div(at + j, 128), lax.rem(at + j, 128)) for j in range(size + 1)]
    codes = [plan[line, lane] for line, lane in lines]
    for j in range(size):
        if size > 1:
            push(bits, codes[j + 1], windows, len(accs), (j + 1) % 2)
        index, _, lattice = unpacked(bits, codes[j])
        other, _, other_lattice = unpacked(bits, plan[blocks + lines[j][0], lines[j][1]])
        tile = tiles[index].astype(jnp.float32)
        beside = tiles[other].astype(jnp.float32)
        for k, acc in enumerate(accs):
            cosine, sine = [weights[2 * k + part, lattice] * tile + weights[2 * k + part, other_lattice] * beside
                            for part in range(2)]
            pltpu.matmul_acc_lhs(acc, matrix_of(cosine, sine), load_staged_rhs=j % 2)
    if size == 1:
        push(bits, codes[1], windows, len(accs), 0)


def every_row(bits, size, row_tiles, first, plan, weights, tiles, windows, accs, spare, finish, done=None):
    kpoints = windows[0].shape[0]
    sets = (accs[:kpoints], accs[kpoints:])
    starts = plan.shape[0] - 1

    def one(row, now, before):
        base = plan[starts, first + row]
        groups = lax.div(plan[starts, first + row + 1] - base, size)
        group(bits, size, base, plan, weights, tiles, windows, now)
        finish(jnp.maximum(row - 1, 0), [pltpu.matmul_pop(acc) for acc in before])
        if done is not None:
            @pl.when(row > 0)
            def _():
                done(row - 1)

        def step(g, _):
            group(bits, size, base + g * size, plan, weights, tiles, windows, now)
            return 0

        lax.fori_loop(1, groups, step, 0)

    def pair(i, _):
        one(2 * i, sets[0], sets[1])
        one(2 * i + 1, sets[1], sets[0])
        return 0

    at = plan[starts, first]
    push(bits, plan[lax.div(at, 128), lax.rem(at, 128)], windows, kpoints, 0)
    lax.fori_loop(0, row_tiles // 2, pair, 0)
    if row_tiles % 2:
        one(row_tiles - 1, sets[0], sets[1])
    finish(row_tiles - 1, [pltpu.matmul_pop(acc) for acc in sets[1 - row_tiles % 2]])
    if done is not None:
        done(row_tiles - 1)
    nothing = jnp.zeros((spare[0].shape[0], 256), jnp.bfloat16)
    for acc in spare:
        pltpu.matmul_acc_lhs(acc, nothing, load_staged_rhs=0)
        pltpu.matmul_pop(acc)


def accumulators(kpoints, edge, vec_count):
    return ([pltpu.ACC(k % 2)((2 * edge, vec_count), jnp.float32) for k in range(kpoints)] * 2
            + [pltpu.ACC(k % 2)((16, vec_count), jnp.float32) for k in range(kpoints)])


def first_kernel(bits, plan, weights, tiles, window, total):
    kpoints, _, row_tiles, edge, vec_count = total.shape

    def run(*accs):
        def finish(row, results):
            for k, result in enumerate(results):
                for part in range(2):
                    total[k, part, row] = result[part * edge:(part + 1) * edge]

        every_row(bits, GROUP, row_tiles, 0, plan, weights, tiles, [window], accs[:-kpoints], accs[-kpoints:], finish)

    pl.run_scoped(run, *accumulators(kpoints, edge, vec_count))


def late_kernel(bits, stage_number, last, plan, weights, tiles, total, across, beside, out, *scratch):
    kpoints, _, row_tiles, edge, vec_count = total.shape
    stage, out_sem = scratch if last else (out, None)

    def store(row):
        return pltpu.make_async_copy(stage.at[:, :, row], out.at[:, :, row], out_sem.at[row])

    def run(*accs):
        def finish(row, results):
            for k, result in enumerate(results):
                for part in range(2):
                    stage[k, part, row] = total[k, part, row] + result[part * edge:(part + 1) * edge]

        every_row(bits, LATE_GROUP, row_tiles, stage_number * row_tiles, plan, weights, tiles, [across, beside],
                  accs[:-kpoints], accs[-kpoints:], finish, (lambda row: store(row).start()) if last else None)

    pl.run_scoped(run, *accumulators(kpoints, edge, vec_count))
    if last:
        for row in range(row_tiles):
            store(row).wait()


def in_hbm(x):
    return pltpu.with_memory_space_constraint(x, pltpu.HBM)


def in_vmem(x):
    return pltpu.with_memory_space_constraint(x, pltpu.VMEM)


def first_product(bits, row_tiles, plan, weights, hop, win):
    kpoints, _, _, edge, vec_count = win.shape
    work = hop.shape[0] * kpoints * 8 * edge * edge * vec_count
    return pl.pallas_call(
        functools.partial(first_kernel, bits),
        out_shape=pltpu.VMEM((kpoints, 2, row_tiles, edge, vec_count), jnp.float32),
        in_specs=[SMEM] * 2 + [VMEM] * 2,
        out_specs=VMEM,
        compiler_params=pltpu.CompilerParams(vmem_limit_bytes=2**20),
        cost_estimate=pl.CostEstimate(flops=work, bytes_accessed=2**24, transcendentals=0),
        name="first",
    )(plan, weights, in_vmem(hop), in_vmem(win))


def late_product(bits, number, last, plan, weights, hop, total, across, beside):
    row_tiles = total.shape[2]
    work = hop.shape[0] * total.size // 2
    return pl.pallas_call(
        functools.partial(late_kernel, bits, number, last),
        out_shape=(jax.ShapeDtypeStruct if last else pltpu.VMEM)(total.shape, jnp.float32),
        in_specs=[SMEM] * 2 + [VMEM] * 4,
        out_specs=ANY if last else VMEM,
        scratch_shapes=[
            pltpu.VMEM(total.shape, jnp.float32),
            pltpu.SemaphoreType.DMA((row_tiles,)),
        ] if last else [],
        compiler_params=pltpu.CompilerParams(vmem_limit_bytes=(12 if last else 2) * 2**20),
        cost_estimate=pl.CostEstimate(flops=work, bytes_accessed=2**22, transcendentals=0),
        name="late",
    )(plan, weights, in_vmem(hop), in_vmem(total), in_vmem(across), in_vmem(beside))


def body(hoppings, tile_rows, tile_cols, tile_lats, tile_counts, phase_angle, vectors):
    edge = hoppings.shape[2]
    group_size = lax.axis_size("ka")
    row_shards = lax.axis_size("rows")
    kpoints, _, orbitals, vec_count = vectors.shape
    lattices = phase_angle.shape[1]
    row_tiles = orbitals // edge
    bits = (bits_of(group_size * hoppings.shape[1]), bits_of(row_tiles + 2 * BAND))
    vec = vectors.reshape(kpoints, 2, row_tiles, edge, vec_count)
    weights = jnp.stack([jnp.cos(phase_angle), jnp.sin(phase_angle)], axis=1).reshape(2 * kpoints, lattices)
    weights = jnp.pad(weights, ((0, 0), (1, 0)))

    ints = (tile_rows, tile_cols, tile_lats, tile_counts)
    all_hop, plan, win, *late = exchange(group_size, row_shards, bits, hoppings[0], ints, vec)
    sign = [1 - 2 * (r % 2) for r in range(row_shards)]
    far = [(r, (r + 2 * sign[r]) % row_shards) for r in range(row_shards)]
    pairs = [(r, r + sign[r]) for r in range(row_shards)]
    moved = [lax.ppermute(x, "rows", pairs if n % 2 else far) for n, x in enumerate(late)]
    total = first_product(bits, row_tiles, plan, weights, all_hop, win)
    for n in range(0, len(moved), 2):
        total = late_product(bits, n // 2 + 1, n + 2 == len(moved), plan, weights, all_hop, total, *moved[n:n + 2])
    return total.reshape(kpoints, 2, orbitals, vec_count)


def solution(mesh):
    return jax.shard_map(
        body,
        mesh=mesh,
        in_specs=(
            P("rows", "ka", None, None),
            P("rows", "ka"),
            P("rows", "ka"),
            P("rows", "ka"),
            P("rows", "ka"),
            P("ka", None),
            P("ka", None, "rows", None),
        ),
        out_specs=P("ka", None, "rows", None),
        check_vma=False,
    )
```

```python
import functools

import jax
import jax.numpy as jnp
from jax import lax
from jax.experimental import pallas as pl
from jax.experimental.pallas import tpu as pltpu
from jax.sharding import PartitionSpec as P

NLAT = 9
BAND = 16
GROUP = 4
LATE_GROUP = 1
MESH = pl.DeviceIdType.MESH


def spans(total, size):
    return [(start, min(size, total - start)) for start in range(0, total, size)]


def late_stages(row_tiles, row_shards):
    reach = (BAND + row_tiles - 1) // row_tiles
    if row_tiles > BAND or row_shards % 2 or reach < 2:
        return []
    extra = min(row_tiles, BAND - row_tiles, row_tiles - 2)
    late = min(extra, row_tiles - extra)
    first = late - late // 2
    stages = [(row_tiles - extra - late, first, 0, extra - extra // 2)]
    if late // 2 and extra // 2:
        stages.append((row_tiles - extra - late // 2, late // 2, extra - extra // 2, extra // 2))
    else:
        stages = [(row_tiles - extra - late, late, 0, extra)]
    return stages


def column(row):
    size = row.shape[1]
    same = (lax.broadcasted_iota(jnp.int32, (size, size), 0) == lax.broadcasted_iota(jnp.int32, (size, size), 1))
    return jnp.sum(jnp.where(same, jnp.broadcast_to(row, (size, size)), 0.0), axis=1, keepdims=True)


def make_plan(row_shards, row_tiles, bits, ints, lives, plan):
    group_size, _, _, per_device = ints.shape
    stages = late_stages(row_tiles, row_shards)
    dead = (len(stages) + 1) * row_tiles
    shard = lax.axis_index("rows")
    row_start = shard * row_tiles
    total_tiles = row_tiles * row_shards
    odd = lax.rem(shard, 2)
    even = 1 - odd
    low, high = BAND - row_tiles, BAND + 2 * row_tiles
    extra = sum(stage[3] for stage in stages)
    main = row_tiles - extra
    ranges = []
    for number, (across_at, across_tiles, beside_at, beside_tiles) in enumerate(stages):
        ranges.append((number + 1, 0, across_tiles,
                       even * (low + main - across_at - across_tiles) + odd * (high - main + across_at)))
        ranges.append((number + 1, across_tiles, beside_tiles,
                       even * (high - extra + beside_at) + odd * (low + extra - beside_at - beside_tiles)))
    lane = lax.broadcasted_iota(jnp.int32, (1, per_device), 1)

    rows, keys, row_cols, key_cols, code_cols = [], [], [], [], []
    for owner in range(group_size):
        place = ints[owner, 1] - row_start + BAND
        place = jnp.where(place < 0, place + total_tiles, place)
        place = jnp.where(place >= total_tiles, place - total_tiles, place)
        row = ints[owner, 0] - row_start
        inside = place
        for number, shift, count, begin in ranges:
            late = (inside >= begin) & (inside < begin + count)
            row = jnp.where(late, row + number * row_tiles, row)
            place = jnp.where(late, inside - begin + shift, place)
        row = jnp.where(lane < lives[owner], row, dead)
        code = (((ints[owner, 2] + 1) << bits[1]) + place << bits[0]) + owner * per_device + lane
        rows.append(row.astype(jnp.float32))
        keys.append(((row << bits[1]) + place).astype(jnp.float32))
        row_cols.append(column(rows[-1]))
        key_cols.append(column(keys[-1]))
        code_cols.append(column(code.astype(jnp.float32)))
    row_col = jnp.concatenate(row_cols, axis=0)
    key_col = jnp.concatenate(key_cols, axis=0)
    code_col = jnp.concatenate(code_cols, axis=0)
    slots = group_size * per_device
    buckets = -(-(dead + 1) // 8) * 8
    bucket = lax.broadcasted_iota(jnp.int32, (buckets, 1), 0).astype(jnp.float32)
    index = lax.broadcasted_iota(jnp.int32, (slots, 1), 0)
    orders, leads = [], []
    for owner, key in enumerate(keys):
        ahead = (key_col == key) & (index < lane + owner * per_device)
        order = jnp.sum(jnp.where(ahead, 1.0, 0.0), axis=0, keepdims=True)
        live = rows[owner] < dead
        orders.append(order)
        leads.append(jnp.where(live & (order - 2 * jnp.floor(order * 0.5) == 0), 1.0, 0.0))
    order_col = jnp.concatenate([column(order) for order in orders], axis=0)
    lead_col = jnp.concatenate([column(lead) for lead in leads], axis=0)

    held = jnp.zeros((buckets, 1), jnp.float32)
    for row, lead in zip(rows, leads):
        held += jnp.sum(jnp.where(bucket == row, lead, 0.0), axis=1, keepdims=True)
    held = jnp.maximum(held, 1.0)
    held = jnp.where(bucket < row_tiles, jnp.floor((held + (GROUP - 1)) * (1 / GROUP)) * GROUP,
                     jnp.floor((held + (LATE_GROUP - 1)) * (1 / LATE_GROUP)) * LATE_GROUP)
    spots = []
    for owner, (row, lead) in enumerate(zip(rows, leads)):
        ahead = (row_col == row) & (index < lane + owner * per_device)
        rank = jnp.sum(jnp.where(ahead, lead_col, 0.0), axis=0, keepdims=True)
        base = jnp.sum(jnp.where(bucket < row, held, 0.0), axis=0, keepdims=True)
        spots.append(column(jnp.where(lead > 0, base + rank, -1.0)))
    spot = jnp.concatenate(spots, axis=0)
    seconds = []
    for row, key, order, lead in zip(rows, keys, orders, leads):
        led = (key_col == key) & (order_col == order - 1)
        found = jnp.sum(jnp.where(led, spot, 0.0), axis=0, keepdims=True)
        seconds.append(column(jnp.where((lead == 0) & (row < dead), found, -1.0)))
    second = jnp.concatenate(seconds, axis=0)
    wide = lax.broadcasted_iota(jnp.int32, (1, 128), 1)
    blocks = (plan.shape[0] - 1) // 2
    for block in range(blocks):
        here = (wide + block * 128).astype(jnp.float32)
        for line, place in ((block, spot), (blocks + block, second)):
            picked = jnp.sum(jnp.where(place == here, code_col, 0.0), axis=0, keepdims=True)
            plan[line:line + 1] = picked.astype(jnp.int32)
    starts = jnp.sum(jnp.where(bucket < wide.astype(jnp.float32), held, 0.0), axis=0, keepdims=True)
    plan[plan.shape[0] - 1:] = starts.astype(jnp.int32)


def exchange_kernel(group_size, row_shards, bits, hop, tile_rows, tile_cols, tile_lats, tile_counts, vec,
                    all_hop, plan, win, *rest):
    stages = late_stages(vec.shape[2], row_shards)
    across_tiles = sum(stage[1] for stage in stages)
    beside_tiles = sum(stage[3] for stage in stages)
    outs, (ints, lives, own_lives, send_sem, recv_sem, local_sem) = rest[:2 * len(stages)], rest[2 * len(stages):]

    slots = hop.shape[0]
    row_tiles = vec.shape[2]
    own_lives[...] = jnp.full(own_lives.shape, tile_counts[0, 0], jnp.int32)
    ka = lax.axis_index("ka")
    row = lax.axis_index("rows")
    odd = lax.rem(row, 2)
    even = 1 - odd
    sign = 1 - 2 * odd
    partner = ka + 1 - 2 * lax.rem(ka, 2)
    reach = (BAND + row_tiles - 1) // row_tiles
    depth_of = lambda d: min(row_tiles, BAND - (d - 1) * row_tiles)

    def at_row(step):
        return {"ka": ka, "rows": lax.rem(row + step + 2 * row_shards, row_shards)}

    def at_ka(other):
        return {"ka": other, "rows": row}

    across = [lax.rem(ka + 2 * h, group_size) for h in range(1, group_size // 2)]
    others = [lax.rem(ka + h, group_size) for h in range(1, group_size)]
    forwarding = row_tiles <= BAND and row_shards % 2 == 0 and reach >= 2
    peers = [at_ka(o) for o in others]
    if forwarding:
        peers.append(at_row(sign))
    else:
        peers += [at_row(1), at_row(-1)]
    for d in range(2, reach + 1):
        peers += [at_row(d), at_row(-d)]

    barrier = pltpu.get_barrier_semaphore()
    for peer in peers:
        pl.semaphore_signal(barrier, inc=1, device_id=peer, device_id_type=MESH)

    local = [
        pltpu.make_async_copy(hop, all_hop.at[pl.ds(ka * slots, slots)], local_sem.at[0]),
        pltpu.make_async_copy(own_lives, lives.at[ka], local_sem.at[1]),
        pltpu.make_async_copy(vec, win.at[:, :, pl.ds(BAND, row_tiles)], local_sem.at[2]),
    ]
    for field, source in enumerate((tile_rows, tile_cols, tile_lats)):
        local.append(pltpu.make_async_copy(source, ints.at[ka, field], local_sem.at[4 + field]))
    for copy in [local[0]] + local[2:]:
        copy.start()
    pl.semaphore_wait(barrier, len(peers))
    local[1].start()

    made = []

    def send(src, dst, device):
        n = len(made)
        copy = pltpu.make_async_remote_copy(
            src_ref=src, dst_ref=dst, send_sem=send_sem.at[n], recv_sem=recv_sem.at[n],
            device_id=device, device_id_type=MESH)
        copy.start()
        made.append(copy)
        return copy

    received = set()

    def arrived(copy):
        copy.wait_recv()
        received.add(id(copy))

    def vec_send(tile, count, step):
        send_to = -step * row_tiles + tile + BAND
        return send(vec.at[:, :, pl.ds(tile, count)], win.at[:, :, pl.ds(send_to, count)], at_row(step))

    def vec_pass(source, tile, count, step):
        here = source * row_tiles + tile + BAND
        there = (source - step) * row_tiles + tile + BAND
        return send(win.at[:, :, pl.ds(here, count)], win.at[:, :, pl.ds(there, count)], at_row(step))

    about = []
    for other in others:
        for field, source in enumerate((tile_rows, tile_cols, tile_lats)):
            about.append(send(source, ints.at[ka, field], at_ka(other)))
        about.append(send(own_lives, lives.at[ka], at_ka(other)))

    near_parts = []
    if forwarding:
        second = depth_of(2)
        extra = min(second, row_tiles - 2)
        main = row_tiles - extra
        kept = main - across_tiles
        parts = [(start, count, None) for start, count in spans(kept, 2)]
        for number, (at, tiles, _, _) in enumerate(stages):
            parts += [(at + start, count, number) for start, count in spans(tiles, 2)]

        def part_tile(parity_even, parity_odd, start, count):
            return parity_even * (extra + start) + parity_odd * (main - start - count)

        near_parts.append(vec_send(part_tile(even, odd, *parts[0][:2]), parts[0][1], sign))
        turned = vec_send(odd * (row_tiles - extra), extra, -2 * sign) if extra else None
    hop_parts = []
    size = max(1, slots // 8)
    hop_spans = spans(slots - size, size)
    start = slots - size
    while start < slots:
        size = min((size + 1) // 2, slots - start)
        hop_spans.append((start, size))
        start += size
    for h, other in enumerate(across):
        for start, count in hop_spans:
            hop_parts.append((ka + 2 * (h + 1), start, count, send(
                hop.at[pl.ds(start, count)], all_hop.at[pl.ds(ka * slots + start, count)], at_ka(other))))
    if forwarding:
        for start, count, _ in parts[1:]:
            near_parts.append(vec_send(part_tile(even, odd, start, count), count, sign))
        if extra and not beside_tiles:
            vec_send(odd * (row_tiles - extra), extra, sign)
        vec_send(even * (row_tiles - second), second, 2 * sign)
        if second > extra:
            vec_send(even * extra + odd * (row_tiles - second), second - extra, -2 * sign)
    else:
        first = depth_of(1)
        vec_send(0, first, -1)
        vec_send(row_tiles - first, first, 1)
        if reach >= 2:
            vec_send(0, depth_of(2), -2)
            vec_send(row_tiles - depth_of(2), depth_of(2), 2)
    for d in range(3, reach + 1):
        vec_send(0, depth_of(d), -d)
        vec_send(row_tiles - depth_of(d), depth_of(d), d)
    for start, count in hop_spans:
        send(hop.at[pl.ds(start, count)], all_hop.at[pl.ds(ka * slots + start, count)], at_ka(partner))

    def pass_hop(n):
        owner, start, count, copy = hop_parts[n]
        owner = lax.rem(owner, group_size)
        arrived(copy)
        block = all_hop.at[pl.ds(owner * slots + start, count)]
        send(block, block, at_ka(partner))

    holds = []
    if stages:
        local[2].wait()
        for number, (_, _, at, count) in enumerate(stages):
            tile = even * (beside_tiles - at - count) + odd * (row_tiles - beside_tiles + at)
            holds.append(pltpu.make_async_copy(
                win.at[:, :, pl.ds(BAND + tile, count)], outs[2 * number + 1], local_sem.at[7 + number]))
            holds[-1].start()

    for copy in about:
        arrived(copy)
    for copy in [local[1]] + local[3:]:
        copy.wait()
    local = [local[0]] + (holds or [local[2]])
    make_plan(row_shards, row_tiles, bits, ints, lives, plan)

    done = 0
    if forwarding:
        for n, copy in enumerate(near_parts):
            arrived(copy)
            start, count, number = parts[n]
            tile = part_tile(odd, even, start, count)
            if number is None:
                vec_pass(sign, tile, count, 2 * sign)
            else:
                first = part_tile(odd, even, *stages[number][:2])
                hold = pltpu.make_async_copy(
                    win.at[:, :, pl.ds(sign * row_tiles + tile + BAND, count)],
                    outs[2 * number].at[:, :, pl.ds(tile - first, count)], local_sem.at[10 + n])
                hold.start()
                local.append(hold)
            if n == 1 and extra:
                arrived(turned)
                vec_pass(2 * sign, odd * (row_tiles - extra), extra, sign)
            until = len(hop_parts) * (n + 1) // (len(near_parts) + 1)
            while done < until:
                pass_hop(done)
                done += 1
        if len(near_parts) < 2 and extra:
            arrived(turned)
            vec_pass(2 * sign, odd * (row_tiles - extra), extra, sign)
    while done < len(hop_parts):
        pass_hop(done)
        done += 1

    for copy in local:
        copy.wait()
    for copy in made:
        if id(copy) not in received:
            copy.wait_recv()
    for copy in made:
        copy.wait_send()


SMEM = pl.BlockSpec(memory_space=pltpu.SMEM)
VMEM = pl.BlockSpec(memory_space=pltpu.VMEM)
ANY = pl.BlockSpec(memory_space=pl.ANY)


def exchange(group_size, row_shards, bits, hop, ints, vec):
    slots = hop.shape[0]
    per_device = ints[0].shape[1]
    row_tiles = vec.shape[2]
    blocks = (group_size * per_device + row_tiles * (GROUP + 2 * LATE_GROUP)) // 128 + 1
    width = vec.shape[2] + 2 * BAND
    stages = late_stages(row_tiles, row_shards)
    late = tuple(
        jax.ShapeDtypeStruct(vec.shape[:2] + (count,) + vec.shape[3:], vec.dtype)
        for _, across, _, beside in stages for count in (across, beside))
    return pl.pallas_call(
        functools.partial(exchange_kernel, group_size, row_shards, bits),
        out_shape=(
            pltpu.VMEM((group_size * slots,) + hop.shape[1:], hop.dtype),
            pltpu.VMEM((2 * blocks + 1, 128), jnp.int32),
            pltpu.VMEM(vec.shape[:2] + (width,) + vec.shape[3:], vec.dtype),
        ) + late,
        in_specs=[ANY] * 4 + [SMEM, ANY],
        out_specs=(pl.BlockSpec(memory_space=pltpu.VMEM), pl.BlockSpec(memory_space=pltpu.VMEM),
                   pl.BlockSpec(memory_space=pltpu.VMEM)) + (pl.BlockSpec(memory_space=pl.ANY),) * len(late),
        scratch_shapes=[
            pltpu.VMEM((group_size, 3, 1, per_device), jnp.int32),
            pltpu.VMEM((group_size, 1, per_device), jnp.int32),
            pltpu.VMEM((1, per_device), jnp.int32),
            pltpu.SemaphoreType.DMA((104,)),
            pltpu.SemaphoreType.DMA((104,)),
            pltpu.SemaphoreType.DMA((24,)),
        ],
        compiler_params=pltpu.CompilerParams(
            collective_id=0, has_side_effects=True, vmem_limit_bytes=4 * 2**20),
        name="exchange",
    )(in_hbm(hop), *map(in_hbm, ints[:3]), ints[3], in_hbm(vec))


def bits_of(count):
    return max(1, (count - 1).bit_length())


def matrix_of(cosine, sine):
    cosine, sine = cosine.astype(jnp.bfloat16), sine.astype(jnp.bfloat16)
    return jnp.concatenate(
        [jnp.concatenate([cosine, -sine], axis=1), jnp.concatenate([sine, cosine], axis=1)], axis=0)


def unpacked(bits, code):
    tile_bits, place_bits = bits
    return (code & (2**tile_bits - 1), (code >> tile_bits) & (2**place_bits - 1),
            code >> (tile_bits + place_bits))


def push(bits, code, windows, kpoints, register):
    _, place, _ = unpacked(bits, code)
    for k in range(kpoints):
        if len(windows) == 1:
            parts = [windows[0][k, part, place] for part in range(2)]
        else:
            split = windows[0].shape[2]
            near, far = jnp.minimum(place, split - 1), jnp.maximum(place - split, 0)
            parts = [jnp.where(place < split, windows[0][k, part, near], windows[1][k, part, far])
                     for part in range(2)]
        pltpu.matmul_push_rhs(jnp.concatenate(parts, axis=0), staging_register=register, mxu_index=k % 2)


def group(bits, size, at, plan, weights, tiles, windows, accs):
    blocks = (plan.shape[0] - 1) // 2
    lines = [(lax.div(at + j, 128), lax.rem(at + j, 128)) for j in range(size + 1)]
    codes = [plan[line, lane] for line, lane in lines]
    for j in range(size):
        if size > 1:
            push(bits, codes[j + 1], windows, len(accs), (j + 1) % 2)
        index, _, lattice = unpacked(bits, codes[j])
        other, _, other_lattice = unpacked(bits, plan[blocks + lines[j][0], lines[j][1]])
        tile = tiles[index].astype(jnp.float32)
        beside = tiles[other].astype(jnp.float32)
        for k, acc in enumerate(accs):
            cosine, sine = [weights[2 * k + part, lattice] * tile + weights[2 * k + part, other_lattice] * beside
                            for part in range(2)]
            pltpu.matmul_acc_lhs(acc, matrix_of(cosine, sine), load_staged_rhs=j % 2)
    if size == 1:
        push(bits, codes[1], windows, len(accs), 0)


def every_row(bits, size, row_tiles, first, plan, weights, tiles, windows, accs, spare, finish, done=None):
    kpoints = windows[0].shape[0]
    sets = (accs[:kpoints], accs[kpoints:])
    starts = plan.shape[0] - 1

    def one(row, now, before):
        base = plan[starts, first + row]
        groups = lax.div(plan[starts, first + row + 1] - base, size)
        group(bits, size, base, plan, weights, tiles, windows, now)
        finish(jnp.maximum(row - 1, 0), [pltpu.matmul_pop(acc) for acc in before])
        if done is not None:
            @pl.when(row > 0)
            def _():
                done(row - 1)

        def step(g, _):
            group(bits, size, base + g * size, plan, weights, tiles, windows, now)
            return 0

        lax.fori_loop(1, groups, step, 0)

    def pair(i, _):
        one(2 * i, sets[0], sets[1])
        one(2 * i + 1, sets[1], sets[0])
        return 0

    at = plan[starts, first]
    push(bits, plan[lax.div(at, 128), lax.rem(at, 128)], windows, kpoints, 0)
    lax.fori_loop(0, row_tiles // 2, pair, 0)
    if row_tiles % 2:
        one(row_tiles - 1, sets[0], sets[1])
    finish(row_tiles - 1, [pltpu.matmul_pop(acc) for acc in sets[1 - row_tiles % 2]])
    if done is not None:
        done(row_tiles - 1)
    nothing = jnp.zeros((spare[0].shape[0], 256), jnp.bfloat16)
    for acc in spare:
        pltpu.matmul_acc_lhs(acc, nothing, load_staged_rhs=0)
        pltpu.matmul_pop(acc)


def accumulators(kpoints, edge, vec_count):
    return ([pltpu.ACC(k % 2)((2 * edge, vec_count), jnp.float32) for k in range(kpoints)] * 2
            + [pltpu.ACC(k % 2)((16, vec_count), jnp.float32) for k in range(kpoints)])


def first_kernel(bits, plan, weights, tiles, window, total):
    kpoints, _, row_tiles, edge, vec_count = total.shape

    def run(*accs):
        def finish(row, results):
            for k, result in enumerate(results):
                for part in range(2):
                    total[k, part, row] = result[part * edge:(part + 1) * edge]

        every_row(bits, GROUP, row_tiles, 0, plan, weights, tiles, [window], accs[:-kpoints], accs[-kpoints:], finish)

    pl.run_scoped(run, *accumulators(kpoints, edge, vec_count))


def late_kernel(bits, stage_number, last, plan, weights, tiles, total, across, beside, out, *scratch):
    kpoints, _, row_tiles, edge, vec_count = total.shape
    stage, out_sem = scratch if last else (out, None)

    def store(row):
        return pltpu.make_async_copy(stage.at[:, :, row], out.at[:, :, row], out_sem.at[row])

    def run(*accs):
        def finish(row, results):
            for k, result in enumerate(results):
                for part in range(2):
                    stage[k, part, row] = total[k, part, row] + result[part * edge:(part + 1) * edge]

        every_row(bits, LATE_GROUP, row_tiles, stage_number * row_tiles, plan, weights, tiles, [across, beside],
                  accs[:-kpoints], accs[-kpoints:], finish, (lambda row: store(row).start()) if last else None)

    pl.run_scoped(run, *accumulators(kpoints, edge, vec_count))
    if last:
        for row in range(row_tiles):
            store(row).wait()


def in_hbm(x):
    return pltpu.with_memory_space_constraint(x, pltpu.HBM)


def in_vmem(x):
    return pltpu.with_memory_space_constraint(x, pltpu.VMEM)


def first_product(bits, row_tiles, plan, weights, hop, win):
    kpoints, _, _, edge, vec_count = win.shape
    work = hop.shape[0] * kpoints * 8 * edge * edge * vec_count
    return pl.pallas_call(
        functools.partial(first_kernel, bits),
        out_shape=pltpu.VMEM((kpoints, 2, row_tiles, edge, vec_count), jnp.float32),
        in_specs=[SMEM] * 2 + [VMEM] * 2,
        out_specs=VMEM,
        compiler_params=pltpu.CompilerParams(vmem_limit_bytes=2**20),
        cost_estimate=pl.CostEstimate(flops=work, bytes_accessed=2**24, transcendentals=0),
        name="first",
    )(plan, weights, in_vmem(hop), in_vmem(win))


def late_product(bits, number, last, plan, weights, hop, total, across, beside):
    row_tiles = total.shape[2]
    work = hop.shape[0] * total.size // 2
    return pl.pallas_call(
        functools.partial(late_kernel, bits, number, last),
        out_shape=(jax.ShapeDtypeStruct if last else pltpu.VMEM)(total.shape, jnp.float32),
        in_specs=[SMEM] * 2 + [VMEM] * 4,
        out_specs=ANY if last else VMEM,
        scratch_shapes=[
            pltpu.VMEM(total.shape, jnp.float32),
            pltpu.SemaphoreType.DMA((row_tiles,)),
        ] if last else [],
        compiler_params=pltpu.CompilerParams(vmem_limit_bytes=(12 if last else 2) * 2**20),
        cost_estimate=pl.CostEstimate(flops=work, bytes_accessed=2**22, transcendentals=0),
        name="late",
    )(plan, weights, in_vmem(hop), in_vmem(total), in_vmem(across), in_vmem(beside))


def body(hoppings, tile_rows, tile_cols, tile_lats, tile_counts, phase_angle, vectors):
    edge = hoppings.shape[2]
    group_size = lax.axis_size("ka")
    row_shards = lax.axis_size("rows")
    kpoints, _, orbitals, vec_count = vectors.shape
    lattices = phase_angle.shape[1]
    row_tiles = orbitals // edge
    bits = (bits_of(group_size * hoppings.shape[1]), bits_of(row_tiles + 2 * BAND))
    vec = vectors.reshape(kpoints, 2, row_tiles, edge, vec_count)
    weights = jnp.stack([jnp.cos(phase_angle), jnp.sin(phase_angle)], axis=1).reshape(2 * kpoints, lattices)
    weights = jnp.pad(weights, ((0, 0), (1, 0)))

    ints = (tile_rows, tile_cols, tile_lats, tile_counts)
    all_hop, plan, win, *late = exchange(group_size, row_shards, bits, hoppings[0], ints, vec)
    sign = [1 - 2 * (r % 2) for r in range(row_shards)]
    far = [(r, (r + 2 * sign[r]) % row_shards) for r in range(row_shards)]
    pairs = [(r, r + sign[r]) for r in range(row_shards)]
    moved = [lax.ppermute(x, "rows", pairs if n % 2 else far) for n, x in enumerate(late)]
    total = first_product(bits, row_tiles, plan, weights, all_hop, win)
    for n in range(0, len(moved), 2):
        total = late_product(bits, n // 2 + 1, n + 2 == len(moved), plan, weights, all_hop, total, *moved[n:n + 2])
    return total.reshape(kpoints, 2, orbitals, vec_count)


def solution(mesh):
    return jax.shard_map(
        body,
        mesh=mesh,
        in_specs=(
            P("rows", "ka", None, None),
            P("rows", "ka"),
            P("rows", "ka"),
            P("rows", "ka"),
            P("rows", "ka"),
            P("ka", None),
            P("ka", None, "rows", None),
        ),
        out_specs=P("ka", None, "rows", None),
        check_vma=False,
    )
```
